768 devices in a mesh: wave: 192 (over y_hi, z, x, core), lev: 4 (over y_lo).
Axes of the slice: x: 4, y: 8 (y_hi: 2, y_lo: 4; y = y_hi * 4 + y_lo), z: 12, core: 2. Of those that a mesh axis runs over, the one named last changes fastest.
Arguments:
- spin_tendency: bfloat16 [384, 2, 136, 768], P('wave', None, 'lev'), may hold values from -6 to 6
- spreading_source: bfloat16 [384, 2, 136, 768], P('wave', None, 'lev'), may hold values from -6 to 6
- heat_source: bfloat16 [384, 2, 136, 768], P('wave', None, 'lev'), may hold values from -6 to 6
- helmholtz_inverses: bfloat16 [4, 192, 136, 136], P('lev', 'wave'), may hold values from -0.5 to 0.5
- heat_spreading_coupler: bfloat16 [136, 136], replicated, may hold values from -0.5 to 0.5
- smoothing_strengths: float32 [136], replicated, may hold values from 0.5 to 30
- azimuthal_order_list: int32 [384], P('wave'), may hold values from 0 to 767
Outputs:
- vorticity_new: bfloat16 [384, 2, 136, 768], P('wave', None, 'lev')
- divergence_new: bfloat16 [384, 2, 136, 768], P('wave', None, 'lev')
- temperature_new: bfloat16 [384, 2, 136, 768], P('wave', None, 'lev')
The draws below stay inside these ranges and needn't reach their ends.
All inputs are finite; a program needn't handle non-finite values.
Results may differ from the reference program's by a relative error of at most 0.0075.
Values may be sent and summed in bfloat16 or wider, within the bound.
No kernel may reach another device: no remote copies, remote signals or barrier semaphores. Data moves between devices by JAX's collectives and lax.ppermute only.
A program may use at most 64 MiB of HBM per device.

```python
import math
import jax
import jax.numpy as jnp
from jax import lax

DEGREE_LIMIT = 768
STRATA_NUMBER = 136
ORDER_ENTRIES = 384
NQ = 192
N_LEV = 4


def with_ends(drawn, own_key, least, top_value):
    longest = drawn.shape.index(max(drawn.shape))
    spots = []
    for shift in (0, 1):
        where = [jax.random.randint(jax.random.fold_in(own_key, axis), (), 0, length) for axis, length in enumerate(drawn.shape)]
        where[longest] = (where[longest] + shift) % drawn.shape[longest]
        spots.append(tuple(where))
    return drawn.at[spots[0]].set(least).at[spots[1]].set(top_value)


def block_levels(rng, shape, split, low, high):
    loudness, own = 1.0, jax.random.fold_in(rng, 6)
    for position, parts in split:
        steps = jnp.exp(jax.random.uniform(jax.random.fold_in(own, position), (parts,), jnp.float32, low / len(split), high / len(split)))
        loudness = loudness * jnp.repeat(steps, shape[position] // parts).reshape([-1 if axis == position else 1 for axis in range(len(shape))])
    return loudness


def noise(key, extent, scale, most, shards=(), held_as=jnp.bfloat16):
    array = jax.random.normal(key, extent, jnp.float32) * scale
    if len(shards) > 0:
        array = block_levels(key, extent, shards, -0.22, 0.18) * array
    return jnp.clip(array, min=-most, max=most).astype(held_as)


def setup_inputs(seed: int = 0) -> dict:
    key_of = jax.random.split(jax.random.key(seed), 8)
    return {
        "spin_tendency": noise(key_of[0], (ORDER_ENTRIES, 2, STRATA_NUMBER, DEGREE_LIMIT), 1.0, 6.0, ((0, 192), (2, 4))),
        "spreading_source": noise(key_of[1], (ORDER_ENTRIES, 2, STRATA_NUMBER, DEGREE_LIMIT), 1.0, 6.0, ((0, 192), (2, 4))),
        "heat_source": noise(key_of[2], (ORDER_ENTRIES, 2, STRATA_NUMBER, DEGREE_LIMIT), 1.0, 6.0, ((0, 192), (2, 4))),
        "helmholtz_inverses": noise(key_of[3], (N_LEV, NQ, STRATA_NUMBER, STRATA_NUMBER), STRATA_NUMBER ** -0.5, 0.5, ((0, 4), (1, 192))),
        "heat_spreading_coupler": noise(key_of[4], (STRATA_NUMBER, STRATA_NUMBER), STRATA_NUMBER ** -0.5, 0.5),
        "smoothing_strengths": jnp.clip(jnp.exp(jax.random.uniform(key_of[5], (STRATA_NUMBER,), jnp.float32, math.log(0.5), math.log(30.0))), 0.5, 30.0),
        "azimuthal_order_list": with_ends(jax.random.randint(key_of[6], (ORDER_ENTRIES,), 0, DEGREE_LIMIT), jax.random.fold_in(key_of[6], 1), 0, DEGREE_LIMIT - 1).astype(jnp.int32),
    }


def damping_table(smoothing_strengths, wavenumbers):
    scaled = (wavenumbers * (wavenumbers + 1)).astype(jnp.float32) / jnp.float32((DEGREE_LIMIT - 1) * DEGREE_LIMIT)
    return 1.0 / (1.0 + smoothing_strengths.astype(jnp.float32)[:, None] * scaled[None, :] ** 2)


def reference(spin_tendency, spreading_source, heat_source, helmholtz_inverses, heat_spreading_coupler, smoothing_strengths, azimuthal_order_list):
    matrices = helmholtz_inverses.reshape(DEGREE_LIMIT, STRATA_NUMBER, STRATA_NUMBER).astype(jnp.float32)
    blending_matrix = heat_spreading_coupler.astype(jnp.float32)
    wavenumbers = jnp.arange(DEGREE_LIMIT, dtype=jnp.int32)
    damping = damping_table(smoothing_strengths, wavenumbers)

    def lone_order_entry(members):
        rhs_div, rhs_temp, rhs_vort, zonal = members
        answer_fields = jnp.einsum("nkp,cpn->ckn", matrices, rhs_div.astype(jnp.float32)).astype(jnp.bfloat16)
        coupled = jnp.einsum("kp,cpn->ckn", blending_matrix, answer_fields.astype(jnp.float32)).astype(jnp.bfloat16)
        temp_new = (rhs_temp.astype(jnp.float32) - coupled.astype(jnp.float32)).astype(jnp.bfloat16)
        vort_new = (rhs_vort.astype(jnp.float32) * damping[None]).astype(jnp.bfloat16)
        interior_slice = (wavenumbers >= zonal)[None, None, :]
        empty_placeholder = jnp.zeros((), jnp.bfloat16)
        return (jnp.where(interior_slice, vort_new, empty_placeholder), jnp.where(interior_slice, answer_fields, empty_placeholder), jnp.where(interior_slice, temp_new, empty_placeholder))

    spin_updated, spreading_updated, heat_updated = lax.map(lone_order_entry, (spreading_source, heat_source, spin_tendency, azimuthal_order_list))
    return (spin_updated, spreading_updated, heat_updated)
```

```python
import jax
import jax.numpy as jnp
from jax import lax
from jax.sharding import Mesh, PartitionSpec as P

WAVE = ("yh", "z", "x", "c")
PEERS = ("yh", "x", "c", "lev")


def refined(mesh):
    return Mesh(mesh.devices.reshape(2, 12, 4, 2, 4), WAVE + ("lev",))


def damping_table(level_gain, wavenumbers, total_n):
    scaled = (wavenumbers * (wavenumbers + 1)).astype(jnp.float32) / jnp.float32(
        (total_n - 1) * total_n
    )
    return 1.0 / (1.0 + level_gain[:, None] * scaled[None, :] ** 2)


def on_device(
    spin_tendency,
    spreading_source,
    heat_source,
    helmholtz_inverses,
    heat_spreading_coupler,
    smoothing_strengths,
    azimuthal_order_list,
):
    rows, parts, lev_local, total_n = spreading_source.shape
    nyh, nz, nx, nc = (lax.axis_size(a) for a in WAVE)
    nlev = lax.axis_size("lev")
    peers = nyh * nx * nc
    layers = lev_local * nlev
    zero = jnp.zeros((), jnp.bfloat16)

    sent = spreading_source.reshape(rows, parts, lev_local, nlev, nyh, nz, nx, nc)
    sent = sent.transpose(4, 6, 7, 3, 5, 1, 0, 2).reshape(
        peers * nlev, nz, parts, rows * lev_local
    )
    got = lax.all_to_all(sent, PEERS, split_axis=0, concat_axis=0, tiled=True)
    matrices = lax.all_gather(helmholtz_inverses[0, 0], "z", axis=0, tiled=False)

    got = got.reshape(peers, nlev, nz, parts, rows, lev_local)
    columns = got.transpose(2, 1, 5, 0, 3, 4).reshape(nz, layers, peers * parts * rows)
    solved = jnp.einsum(
        "zkp,zpb->zkb", matrices, columns, preferred_element_type=jnp.float32
    ).astype(jnp.bfloat16)
    coupled = jnp.einsum(
        "ok,zkb->zob", heat_spreading_coupler, solved, preferred_element_type=jnp.float32
    ).astype(jnp.bfloat16)
    both = jnp.stack([solved, coupled]).reshape(2, nz, nlev, lev_local, peers, parts, rows)
    both = both.transpose(4, 2, 5, 0, 1, 6, 3).reshape(
        peers * nlev, parts, 2 * nz * rows * lev_local
    )
    back = lax.all_to_all(both, PEERS, split_axis=0, concat_axis=0, tiled=True)
    back = back.reshape(nyh, nx, nc, nlev, parts, 2, nz, rows, lev_local)
    back = back.transpose(5, 7, 4, 8, 3, 0, 6, 1, 2).reshape(
        2, rows, parts, lev_local, total_n
    )
    spreading_updated, coupled_out = back[0], back[1]

    heat_updated = (heat_source.astype(jnp.float32) - coupled_out.astype(jnp.float32)).astype(
        jnp.bfloat16
    )
    level_gain = lax.dynamic_slice_in_dim(
        smoothing_strengths, lax.axis_index("lev") * lev_local, lev_local
    )
    damping = damping_table(level_gain, jnp.arange(total_n, dtype=jnp.int32), total_n)
    spin_updated = (spin_tendency.astype(jnp.float32) * damping[None, None]).astype(jnp.bfloat16)
    interior = (
        jnp.arange(total_n, dtype=jnp.int32)[None, :] >= azimuthal_order_list[:, None]
    )[:, None, None, :]
    return (
        jnp.where(interior, spin_updated, zero),
        jnp.where(interior, spreading_updated, zero),
        jnp.where(interior, heat_updated, zero),
    )


def solution(mesh):
    spectrum = P(WAVE, None, "lev", None)
    return jax.shard_map(
        on_device,
        mesh=refined(mesh),
        in_specs=(spectrum, spectrum, spectrum, P("lev", WAVE, None, None), P(), P(), P(WAVE)),
        out_specs=(spectrum,) * 3,
        check_vma=False,
    )
```

```python
import jax
import jax.numpy as jnp
from jax import lax
from jax.experimental import pallas as pl
from jax.experimental.pallas import tpu as pltpu
from jax.sharding import Mesh, PartitionSpec as P

WAVE = ("yh", "z", "x", "c")
PEERS = ("yh", "x", "c", "lev")
NT = (((1,), (1,)), ((), ()))
NN = (((1,), (0,)), ((), ()))


def refined(mesh):
    return Mesh(mesh.devices.reshape(2, 12, 4, 2, 4), WAVE + ("lev",))


def dot(a, b, dims):
    return lax.dot_general(a, b, dims, preferred_element_type=jnp.float32)


def damping_table(level_gain, wavenumbers, total_n):
    scaled = (wavenumbers * (wavenumbers + 1)).astype(jnp.float32) / jnp.float32(
        (total_n - 1) * total_n
    )
    return 1.0 / (1.0 + level_gain[:, None] * scaled[None, :] ** 2)


def pack_kernel(m_ref, o_ref):
    m = m_ref[...].astype(jnp.float32)
    o_ref[0:136, :] = m[:, 0:128].astype(jnp.bfloat16)
    tail = m[:, 128:136]
    flipped = jnp.concatenate([tail, jnp.zeros((120, 8), jnp.float32)], axis=0)
    flipped = jnp.concatenate([flipped, jnp.zeros((256, 120), jnp.float32)], axis=1).T
    o_ref[136:152, :] = jnp.concatenate(
        [flipped[0:8, 0:128], flipped[0:8, 128:256]], axis=0
    ).astype(jnp.bfloat16)


def solve_kernel(x_ref, m_ref, c_ref, o_ref, stage):
    nz = x_ref.shape[0]
    stage[...] = jnp.zeros_like(stage)
    coupler = c_ref[...]
    for z in range(nz):
        x = x_ref[z]
        tail = m_ref[z, 136:152, :]
        x_tail = x[:, 128:136]
        low = dot(x[:, 0:128], m_ref[z, 0:136, :], NT)
        high = jnp.concatenate(
            [dot(x_tail, tail[0:8, :], NN), dot(x_tail, tail[8:16, 0:8], NN)], axis=1
        )
        solved = (low + high).astype(jnp.bfloat16)
        coupled = dot(solved, coupler, NT).astype(jnp.bfloat16)
        for f, values in enumerate((solved, coupled)):
            values = values.astype(jnp.float32)
            for c in range(2):
                for r in range(2):
                    rows = values[(c * 2 + r) * 16 : (c * 2 + r + 1) * 16, :]
                    at = z * 136 + f * 68 + r * 34
                    for l in range(4):
                        stage[l, c, :, at : at + 34] = rows[:, l * 34 : l * 34 + 34]
    for l in range(4):
        for c in range(2):
            o_ref[l, c] = stage[l, c].astype(jnp.bfloat16)


def finish_kernel(m_ref, b_ref, heat_ref, div_ref, temp_ref, stage):
    spans = []
    for c in range(2):
        flipped = b_ref[c].astype(jnp.float32).T
        spans.append([flipped[z * 136 : (z + 1) * 136, :] for z in range(12)])
    total = None
    for g in range(3):
        sides = []
        for c in range(2):
            s = spans[c][4 * g : 4 * g + 4]
            sides.append(jnp.concatenate(s, axis=1))
        left = jnp.concatenate(sides, axis=0).astype(jnp.bfloat16)
        row = lax.broadcasted_iota(jnp.int32, (256, 768), 0)
        col = lax.broadcasted_iota(jnp.int32, (256, 768), 1)
        z, s, l = 4 * g + (row >> 6), (row >> 2) & 15, row & 3
        place = l * 192 + (s >> 3) * 96 + z * 8 + (s & 7)
        put = jnp.where(col == place, 1.0, 0.0).astype(jnp.bfloat16)
        part = dot(left, put, NN)
        total = part if total is None else total + part
    for c in range(2):
        for t in range(6):
            stage[t, pl.ds(c, 136, 2), :] = total[
                c * 136 : (c + 1) * 136, t * 128 : (t + 1) * 128
            ]
    lane = lax.broadcasted_iota(jnp.int32, (2, 768), 1)
    for r in range(2):
        inside = lane >= m_ref[r]
        for k in range(34):
            at = 2 * (r * 34 + k)
            solved, coupled = (
                jnp.concatenate([stage[t, i : i + 2, :] for t in range(6)], axis=1)
                for i in (at, 136 + at)
            )
            heat = heat_ref[r, k].astype(jnp.float32)
            div_ref[r, k] = jnp.where(inside, solved, 0.0).astype(jnp.bfloat16)
            temp_ref[r, k] = jnp.where(inside, heat - coupled, 0.0).astype(jnp.bfloat16)


def vmem(n):
    return [pl.BlockSpec(memory_space=pltpu.VMEM)] * n


def on_device(
    spin_tendency,
    spreading_source,
    heat_source,
    helmholtz_inverses,
    heat_spreading_coupler,
    smoothing_strengths,
    azimuthal_order_list,
):
    rows, parts, lev_local, total_n = spreading_source.shape
    nyh, nz, nx, nc = (lax.axis_size(a) for a in WAVE)
    nlev = lax.axis_size("lev")
    peers = nyh * nx * nc
    layers = lev_local * nlev
    zero = jnp.zeros((), jnp.bfloat16)

    packed = pl.pallas_call(
        pack_kernel,
        out_shape=jax.ShapeDtypeStruct((layers + 16, 128), jnp.bfloat16),
        in_specs=vmem(1),
        out_specs=vmem(1)[0],
    )(helmholtz_inverses[0, 0])

    sent = spreading_source.reshape(rows, parts, lev_local, nlev, nyh, nz, nx, nc)
    sent = sent.transpose(4, 6, 7, 3, 5, 1, 0, 2).reshape(
        peers * nlev, nz, parts, rows * lev_local
    )
    got = lax.all_to_all(sent, PEERS, split_axis=0, concat_axis=0, tiled=True)
    matrices = lax.all_gather(packed, "z", axis=0, tiled=False)

    got = got.reshape(peers, nlev, nz, parts, rows, lev_local)
    columns = got.transpose(2, 3, 4, 0, 1, 5).reshape(nz, parts * rows * peers, layers)
    width = 13 * 128
    both = pl.pallas_call(
        solve_kernel,
        out_shape=jax.ShapeDtypeStruct((nlev, parts, peers, width), jnp.bfloat16),
        in_specs=vmem(3),
        out_specs=vmem(1)[0],
        scratch_shapes=[pltpu.VMEM((nlev, parts, peers, width), jnp.float32)],
    )(columns, matrices, heat_spreading_coupler)
    both = both.transpose(2, 0, 1, 3).reshape(peers * nlev, parts, width)
    back = lax.all_to_all(both, PEERS, split_axis=0, concat_axis=0, tiled=True)
    back = back.transpose(1, 0, 2)

    out = jax.ShapeDtypeStruct((rows, lev_local, parts, total_n), jnp.bfloat16)
    divergence, temperature = pl.pallas_call(
        finish_kernel,
        out_shape=(out, out),
        in_specs=[pl.BlockSpec(memory_space=pltpu.SMEM)] + vmem(2),
        out_specs=tuple(vmem(2)),
        scratch_shapes=[pltpu.VMEM((total_n // 128, 4 * rows * lev_local, 128), jnp.float32)],
    )(azimuthal_order_list, back, heat_source.transpose(0, 2, 1, 3))

    level_gain = lax.dynamic_slice_in_dim(
        smoothing_strengths, lax.axis_index("lev") * lev_local, lev_local
    )
    damping = damping_table(level_gain, jnp.arange(total_n, dtype=jnp.int32), total_n)
    spin_updated = (spin_tendency.astype(jnp.float32) * damping[None, None]).astype(jnp.bfloat16)
    interior = (
        jnp.arange(total_n, dtype=jnp.int32)[None, :] >= azimuthal_order_list[:, None]
    )[:, None, None, :]
    return (
        jnp.where(interior, spin_updated, zero),
        divergence.transpose(0, 2, 1, 3),
        temperature.transpose(0, 2, 1, 3),
    )


def solution(mesh):
    spectrum = P(WAVE, None, "lev", None)
    return jax.shard_map(
        on_device,
        mesh=refined(mesh),
        in_specs=(spectrum, spectrum, spectrum, P("lev", WAVE, None, None), P(), P(), P(WAVE)),
        out_specs=(spectrum,) * 3,
        check_vma=False,
    )
```

```python
import jax
import jax.numpy as jnp
from jax import lax
from jax.experimental import pallas as pl
from jax.experimental.pallas import tpu as pltpu
from jax.sharding import Mesh, PartitionSpec as P

WAVE = ("yh", "z", "x", "c")
PEERS = ("yh", "x", "c", "lev")
NT = (((1,), (1,)), ((), ()))
NN = (((1,), (0,)), ((), ()))
LIMIT = pltpu.CompilerParams(vmem_limit_bytes=16 * 2**20)


def refined(mesh):
    return Mesh(mesh.devices.reshape(2, 12, 4, 2, 4), WAVE + ("lev",))


def dot(a, b, dims):
    return lax.dot_general(a, b, dims, preferred_element_type=jnp.float32)


def damping_table(level_gain, wavenumbers, total_n):
    scaled = (wavenumbers * (wavenumbers + 1)).astype(jnp.float32) / jnp.float32(
        (total_n - 1) * total_n
    )
    return 1.0 / (1.0 + level_gain[:, None] * scaled[None, :] ** 2)


def pack_matrix(m_ref, o_ref):
    m = m_ref[...].astype(jnp.float32)
    o_ref[0:136, :] = m[:, 0:128].astype(jnp.bfloat16)
    tail = m[:, 128:136]
    flipped = jnp.concatenate([tail, jnp.zeros((120, 8), jnp.float32)], axis=0)
    flipped = jnp.concatenate([flipped, jnp.zeros((256, 120), jnp.float32)], axis=1).T
    o_ref[136:152, :] = jnp.concatenate(
        [flipped[0:8, 0:128], flipped[0:8, 128:256]], axis=0
    ).astype(jnp.bfloat16)


def prepare_kernel(x_ref, m_ref, o_ref, p_ref):
    pack_matrix(m_ref, p_ref)
    x = x_ref[...].astype(jnp.float32)
    sides = []
    for c in range(2):
        rows = jnp.concatenate(
            [x[0, :, c, :], x[1, :, c, :], jnp.zeros((4, 768), jnp.float32)], axis=0
        )
        sides.append(rows.T[:, 0:68])
    both = jnp.stack(sides, axis=1).astype(jnp.bfloat16).reshape(4, 2, 12, 8, 2, 68)
    for l in range(4):
        for yh in range(2):
            for z in range(12):
                o_ref[yh, :, l, z] = both[l, yh, z]


def solve_kernel(x_ref, m_ref, c_ref, o_ref, stage, sol):
    nz = m_ref.shape[0]
    for l in range(4):
        for c in range(2):
            stage[l, c, :, 1536:1664] = jnp.zeros((16, 128), jnp.float32)
    for z in range(nz):
        parts = ([], [])
        for l in range(4):
            got = x_ref[:, l, z].astype(jnp.float32)
            for c in range(2):
                parts[c].append(got[:, c, :])
        x = jnp.concatenate(
            [
                jnp.concatenate(
                    [parts[c][l][:, r * 34 : r * 34 + 34] for l in range(4)], axis=1
                )
                for c in range(2)
                for r in range(2)
            ],
            axis=0,
        ).astype(jnp.bfloat16)
        tail = m_ref[z, 136:152, :]
        x_tail = x[:, 128:136]
        low = dot(x[:, 0:128], m_ref[z, 0:136, :], NT)
        high = jnp.concatenate(
            [dot(x_tail, tail[0:8, :], NN), dot(x_tail, tail[8:16, 0:8], NN)], axis=1
        )
        sol[z * 64 : z * 64 + 64, :] = (low + high).astype(jnp.bfloat16)
    coupled = dot(sol[...], c_ref[...], NT).astype(jnp.bfloat16)
    for z in range(nz):
        both = [
            values[z * 64 : z * 64 + 64, :].astype(jnp.float32) for values in (sol, coupled)
        ]
        for c in range(2):
            for l in range(4):
                stage[l, c, :, z * 136 : z * 136 + 136] = jnp.concatenate(
                    [
                        values[(c * 2 + r) * 16 : (c * 2 + r) * 16 + 16, l * 34 : l * 34 + 34]
                        for values in both
                        for r in range(2)
                    ],
                    axis=1,
                )
    for l in range(4):
        o_ref[:, l] = jnp.stack([stage[l, 0], stage[l, 1]], axis=1).astype(jnp.bfloat16)


def finish_kernel(m_ref, b_ref, heat_ref, div_ref, temp_ref, stage):
    full = b_ref[...].astype(jnp.float32)
    spans = []
    for c in range(2):
        flipped = full[:, c, :].T
        spans.append([flipped[z * 136 : (z + 1) * 136, :] for z in range(12)])
    total = None
    for g in range(3):
        sides = [jnp.concatenate(spans[c][4 * g : 4 * g + 4], axis=1) for c in range(2)]
        left = jnp.concatenate(sides, axis=0).astype(jnp.bfloat16)
        row = lax.broadcasted_iota(jnp.int32, (256, 768), 0)
        col = lax.broadcasted_iota(jnp.int32, (256, 768), 1)
        z, s, l = 4 * g + (row >> 6), (row >> 2) & 15, row & 3
        place = l * 192 + (s >> 3) * 96 + z * 8 + (s & 7)
        put = jnp.where(col == place, 1.0, 0.0).astype(jnp.bfloat16)
        part = dot(left, put, NN)
        total = part if total is None else total + part
    for c in range(2):
        for t in range(6):
            stage[t, pl.ds(c, 136, 2), :] = total[
                c * 136 : (c + 1) * 136, t * 128 : (t + 1) * 128
            ]
    lane = lax.broadcasted_iota(jnp.int32, (2, 768), 1)
    for r in range(2):
        inside = lane >= m_ref[r]
        for k in range(34):
            at = 2 * (r * 34 + k)
            solved, coupled = (
                jnp.concatenate([stage[t, i : i + 2, :] for t in range(6)], axis=1)
                for i in (at, 136 + at)
            )
            heat = heat_ref[r, k].astype(jnp.float32)
            div_ref[r, k] = jnp.where(inside, solved, 0.0).astype(jnp.bfloat16)
            temp_ref[r, k] = jnp.where(inside, heat - coupled, 0.0).astype(jnp.bfloat16)


def vmem(n):
    return [pl.BlockSpec(memory_space=pltpu.VMEM)] * n


def on_device(
    spin_tendency,
    spreading_source,
    heat_source,
    helmholtz_inverses,
    heat_spreading_coupler,
    smoothing_strengths,
    azimuthal_order_list,
):
    rows, parts, lev_local, total_n = spreading_source.shape
    nyh, nz, nx, nc = (lax.axis_size(a) for a in WAVE)
    nlev = lax.axis_size("lev")
    peers = nyh * nx * nc
    layers = lev_local * nlev
    zero = jnp.zeros((), jnp.bfloat16)

    sent, packed = pl.pallas_call(
        prepare_kernel,
        out_shape=(
            jax.ShapeDtypeStruct((nyh, nx * nc, nlev, nz, parts, rows * lev_local), jnp.bfloat16),
            jax.ShapeDtypeStruct((layers + 16, 128), jnp.bfloat16),
        ),
        in_specs=vmem(2),
        out_specs=tuple(vmem(2)),
        compiler_params=LIMIT,
    )(spreading_source.transpose(0, 2, 1, 3), helmholtz_inverses[0, 0])
    sent = sent.reshape(peers * nlev, nz, parts, rows * lev_local)
    got = lax.all_to_all(sent, PEERS, split_axis=0, concat_axis=0, tiled=True)
    matrices = lax.all_gather(packed, "z", axis=0, tiled=False)

    width = 13 * 128
    both = pl.pallas_call(
        solve_kernel,
        out_shape=jax.ShapeDtypeStruct((peers, nlev, parts, width), jnp.bfloat16),
        in_specs=vmem(3),
        out_specs=vmem(1)[0],
        scratch_shapes=[
            pltpu.VMEM((nlev, parts, peers, width), jnp.float32),
            pltpu.VMEM((nz * parts * rows * peers, layers), jnp.bfloat16),
        ],
        compiler_params=LIMIT,
    )(
        got.reshape(peers, nlev, nz, parts, rows * lev_local),
        matrices,
        heat_spreading_coupler,
    )
    both = both.reshape(peers * nlev, parts, width)
    back = lax.all_to_all(both, PEERS, split_axis=0, concat_axis=0, tiled=True)

    out = jax.ShapeDtypeStruct((rows, lev_local, parts, total_n), jnp.bfloat16)
    divergence, temperature = pl.pallas_call(
        finish_kernel,
        out_shape=(out, out),
        in_specs=[pl.BlockSpec(memory_space=pltpu.SMEM)] + vmem(2),
        out_specs=tuple(vmem(2)),
        scratch_shapes=[pltpu.VMEM((total_n // 128, 4 * rows * lev_local, 128), jnp.float32)],
        compiler_params=LIMIT,
    )(azimuthal_order_list, back, heat_source.transpose(0, 2, 1, 3))

    level_gain = lax.dynamic_slice_in_dim(
        smoothing_strengths, lax.axis_index("lev") * lev_local, lev_local
    )
    damping = damping_table(level_gain, jnp.arange(total_n, dtype=jnp.int32), total_n)
    spin_updated = (spin_tendency.astype(jnp.float32) * damping[None, None]).astype(jnp.bfloat16)
    interior = (
        jnp.arange(total_n, dtype=jnp.int32)[None, :] >= azimuthal_order_list[:, None]
    )[:, None, None, :]
    return (
        jnp.where(interior, spin_updated, zero),
        divergence.transpose(0, 2, 1, 3),
        temperature.transpose(0, 2, 1, 3),
    )


def solution(mesh):
    spectrum = P(WAVE, None, "lev", None)
    return jax.shard_map(
        on_device,
        mesh=refined(mesh),
        in_specs=(spectrum, spectrum, spectrum, P("lev", WAVE, None, None), P(), P(), P(WAVE)),
        out_specs=(spectrum,) * 3,
        check_vma=False,
    )
```

```python
import jax
import jax.numpy as jnp
from jax import lax
from jax.experimental import pallas as pl
from jax.experimental.pallas import tpu as pltpu
from jax.sharding import Mesh, PartitionSpec as P

WAVE = ("yh", "zh", "zl", "x", "c")
PEERS = ("yh", "zl", "x", "lev")
SHARERS = ("zh", "c")
NT = (((1,), (1,)), ((), ()))
NN = (((1,), (0,)), ((), ()))
LIMIT = pltpu.CompilerParams(vmem_limit_bytes=16 * 2**20)


def refined(mesh):
    return Mesh(mesh.devices.reshape(2, 6, 2, 4, 2, 4), WAVE + ("lev",))


def dot(a, b, dims):
    return lax.dot_general(a, b, dims, preferred_element_type=jnp.float32)


def damping_table(level_gain, wavenumbers, total_n):
    scaled = (wavenumbers * (wavenumbers + 1)).astype(jnp.float32) / jnp.float32(
        (total_n - 1) * total_n
    )
    return 1.0 / (1.0 + level_gain[:, None] * scaled[None, :] ** 2)


def pack_matrix(m_ref, o_ref):
    m = m_ref[...].astype(jnp.float32)
    o_ref[0:136, :] = m[:, 0:128].astype(jnp.bfloat16)
    tail = m[:, 128:136]
    flipped = jnp.concatenate([tail, jnp.zeros((120, 8), jnp.float32)], axis=0)
    flipped = jnp.concatenate([flipped, jnp.zeros((256, 120), jnp.float32)], axis=1).T
    o_ref[136:152, :] = jnp.concatenate(
        [flipped[0:8, 0:128], flipped[0:8, 128:256]], axis=0
    ).astype(jnp.bfloat16)


def prepare_kernel(x_hbm, m_hbm, o_hbm, p_ref, x_ref, m_ref, o_ref, sems):
    load_m = pltpu.make_async_copy(m_hbm, m_ref, sems.at[0])
    load_m.start()
    load_x = pltpu.make_async_copy(x_hbm, x_ref, sems.at[1])
    load_x.start()
    load_m.wait()
    pack_matrix(m_ref, p_ref)
    load_x.wait()
    leaving = []
    for h in range(2):
        sides = []
        for c in range(2):
            x = x_ref[:, :, :, h * 384 : h * 384 + 384].astype(jnp.float32)
            rows = jnp.concatenate(
                [x[0, :, c, :], x[1, :, c, :], jnp.zeros((4, 384), jnp.float32)], axis=0
            )
            sides.append(rows.T[:, 0:68])
        both = jnp.stack(sides, axis=1).astype(jnp.bfloat16).reshape(2, 2, 6, 2, 4, 2, 2, 68)
        for l in range(2):
            for yh in range(2):
                for zh in range(6):
                    for zl in range(2):
                        o_ref[yh, zl, :, 2 * h + l, zh] = both[l, yh, zh, zl]
        part = pl.ds(2 * h, 2)
        leave = pltpu.make_async_copy(
            o_ref.at[:, :, :, part], o_hbm.at[:, :, :, part], sems.at[2 + h]
        )
        leave.start()
        leaving.append(leave)
    for leave in leaving:
        leave.wait()


def solve_kernel(x_ref, m_ref, c_ref, o_hbm, stage, sol, o_ref, sems):
    nz = m_ref.shape[0]
    for l in range(4):
        for c in range(2):
            stage[l, c, :, 1536:1664] = jnp.zeros((16, 128), jnp.float32)
    for z in range(nz):
        parts = ([], [])
        for l in range(4):
            got = x_ref[:, l, z].astype(jnp.float32)
            for c in range(2):
                parts[c].append(got[:, c, :])
        x = jnp.concatenate(
            [
                jnp.concatenate(
                    [parts[c][l][:, r * 34 : r * 34 + 34] for l in range(4)], axis=1
                )
                for c in range(2)
                for r in range(2)
            ],
            axis=0,
        ).astype(jnp.bfloat16)
        tail = m_ref[z, 136:152, :]
        x_tail = x[:, 128:136]
        low = dot(x[:, 0:128], m_ref[z, 0:136, :], NT)
        high = jnp.concatenate(
            [dot(x_tail, tail[0:8, :], NN), dot(x_tail, tail[8:16, 0:8], NN)], axis=1
        )
        sol[z * 64 : z * 64 + 64, :] = (low + high).astype(jnp.bfloat16)
    coupled = dot(sol[...], c_ref[...], NT).astype(jnp.bfloat16)
    for z in range(nz):
        both = [
            values[z * 64 : z * 64 + 64, :].astype(jnp.float32) for values in (sol, coupled)
        ]
        for c in range(2):
            for l in range(4):
                stage[l, c, :, z * 136 : z * 136 + 136] = jnp.concatenate(
                    [
                        values[(c * 2 + r) * 16 : (c * 2 + r) * 16 + 16, l * 34 : l * 34 + 34]
                        for values in both
                        for r in range(2)
                    ],
                    axis=1,
                )
    leaving = []
    for l in range(4):
        o_ref[:, l] = jnp.stack([stage[l, 0], stage[l, 1]], axis=1).astype(jnp.bfloat16)
        leave = pltpu.make_async_copy(o_ref.at[:, l], o_hbm.at[:, l], sems.at[l])
        leave.start()
        leaving.append(leave)
    for leave in leaving:
        leave.wait()


def place_kernel(q_ref):
    for g in range(3):
        row = lax.broadcasted_iota(jnp.int32, (256, 768), 0)
        col = lax.broadcasted_iota(jnp.int32, (256, 768), 1)
        q, s, l = 4 * g + (row >> 6), (row >> 2) & 15, row & 3
        yh, zl, x = s >> 3, (s >> 2) & 1, s & 3
        place = l * 192 + yh * 96 + (q >> 1) * 16 + zl * 8 + x * 2 + (q & 1)
        q_ref[g * 256 : g * 256 + 256, :] = jnp.where(col == place, 1.0, 0.0).astype(
            jnp.bfloat16
        )


def finish_kernel(
    m_ref, b_ref, heat_ref, q_ref, div_hbm, temp_hbm, stage, div_ref, temp_ref, sems
):
    full = b_ref[...].astype(jnp.float32)
    spans = []
    for c in range(2):
        flipped = full[:, c, :].T
        spans.append([flipped[q * 136 : (q + 1) * 136, :] for q in range(12)])
    total = None
    for g in range(3):
        sides = [jnp.concatenate(spans[c][4 * g : 4 * g + 4], axis=1) for c in range(2)]
        left = jnp.concatenate(sides, axis=0).astype(jnp.bfloat16)
        part = dot(left, q_ref[g * 256 : g * 256 + 256, :], NN)
        total = part if total is None else total + part
    for c in range(2):
        for t in range(6):
            stage[t, pl.ds(c, 136, 2), :] = total[
                c * 136 : (c + 1) * 136, t * 128 : (t + 1) * 128
            ]
    lane = lax.broadcasted_iota(jnp.int32, (2, 768), 1)
    leaving = []
    for r in range(2):
        inside = lane >= m_ref[r]
        for k in range(34):
            at = 2 * (r * 34 + k)
            solved, coupled = (
                jnp.concatenate([stage[t, i : i + 2, :] for t in range(6)], axis=1)
                for i in (at, 136 + at)
            )
            heat = heat_ref[r, k].astype(jnp.float32)
            div_ref[r, k] = jnp.where(inside, solved, 0.0).astype(jnp.bfloat16)
            temp_ref[r, k] = jnp.where(inside, heat - coupled, 0.0).astype(jnp.bfloat16)
        for f, (ready, out) in enumerate(((div_ref, div_hbm), (temp_ref, temp_hbm))):
            leave = pltpu.make_async_copy(ready.at[r], out.at[r], sems.at[2 * r + f])
            leave.start()
            leaving.append(leave)
    for leave in leaving:
        leave.wait()


VMEM = pl.BlockSpec(memory_space=pltpu.VMEM)
SMEM = pl.BlockSpec(memory_space=pltpu.SMEM)
HBM = pl.BlockSpec(memory_space=pltpu.HBM)


def copies(n):
    return pltpu.SemaphoreType.DMA((n,))


def on_device(
    spin_tendency,
    spreading_source,
    heat_source,
    helmholtz_inverses,
    heat_spreading_coupler,
    smoothing_strengths,
    azimuthal_order_list,
):
    rows, parts, lev_local, total_n = spreading_source.shape
    nyh, nzh, nzl, nx, nc = (lax.axis_size(a) for a in WAVE)
    nlev = lax.axis_size("lev")
    peers = nyh * nzl * nx
    shared = nzh * nc
    layers = lev_local * nlev
    zero = jnp.zeros((), jnp.bfloat16)

    def bf16(*shape):
        return jax.ShapeDtypeStruct(shape, jnp.bfloat16)

    def room(*shape, dtype=jnp.bfloat16):
        return pltpu.VMEM(shape, dtype)

    outgoing = (nyh, nzl, nx, nlev, nzh, nc, parts, rows * lev_local)
    sent, packed = pl.pallas_call(
        prepare_kernel,
        out_shape=(bf16(*outgoing), bf16(layers + 16, 128)),
        in_specs=[HBM, HBM],
        out_specs=(HBM, VMEM),
        scratch_shapes=[
            room(rows, lev_local, parts, total_n),
            room(layers, layers),
            room(*outgoing),
            copies(4),
        ],
        compiler_params=LIMIT,
    )(
        pltpu.with_memory_space_constraint(spreading_source.transpose(0, 2, 1, 3), pltpu.HBM),
        pltpu.with_memory_space_constraint(helmholtz_inverses[0, 0], pltpu.HBM),
    )
    sent = sent.reshape(peers * nlev, shared, parts, rows * lev_local)
    got = lax.all_to_all(sent, PEERS, split_axis=0, concat_axis=0, tiled=True)
    matrices = lax.all_gather(packed, SHARERS, axis=0, tiled=False)

    width = 13 * 128
    both = pl.pallas_call(
        solve_kernel,
        out_shape=bf16(peers, nlev, parts, width),
        in_specs=[VMEM] * 3,
        out_specs=HBM,
        scratch_shapes=[
            room(nlev, parts, peers, width, dtype=jnp.float32),
            room(shared * parts * rows * peers, layers),
            room(peers, nlev, parts, width),
            copies(4),
        ],
        compiler_params=LIMIT,
    )(
        got.reshape(peers, nlev, shared, parts, rows * lev_local),
        matrices,
        heat_spreading_coupler,
    )
    both = both.reshape(peers * nlev, parts, width)
    back = lax.all_to_all(both, PEERS, split_axis=0, concat_axis=0, tiled=True)

    places = pl.pallas_call(
        place_kernel, out_shape=bf16(total_n, total_n), out_specs=VMEM, compiler_params=LIMIT
    )()
    spectrum = (rows, lev_local, parts, total_n)
    divergence, temperature = pl.pallas_call(
        finish_kernel,
        out_shape=(bf16(*spectrum), bf16(*spectrum)),
        in_specs=[SMEM] + [VMEM] * 3,
        out_specs=(HBM, HBM),
        scratch_shapes=[
            room(total_n // 128, 4 * rows * lev_local, 128, dtype=jnp.float32),
            room(*spectrum),
            room(*spectrum),
            copies(4),
        ],
        compiler_params=LIMIT,
    )(azimuthal_order_list, back, heat_source.transpose(0, 2, 1, 3), places)

    level_gain = lax.dynamic_slice_in_dim(
        smoothing_strengths, lax.axis_index("lev") * lev_local, lev_local
    )
    damping = damping_table(level_gain, jnp.arange(total_n, dtype=jnp.int32), total_n)
    spin_updated = (spin_tendency.astype(jnp.float32) * damping[None, None]).astype(jnp.bfloat16)
    interior = (
        jnp.arange(total_n, dtype=jnp.int32)[None, :] >= azimuthal_order_list[:, None]
    )[:, None, None, :]
    return (
        jnp.where(interior, spin_updated, zero),
        divergence.transpose(0, 2, 1, 3),
        temperature.transpose(0, 2, 1, 3),
    )


def solution(mesh):
    spectrum = P(WAVE, None, "lev", None)
    return jax.shard_map(
        on_device,
        mesh=refined(mesh),
        in_specs=(spectrum, spectrum, spectrum, P("lev", WAVE, None, None), P(), P(), P(WAVE)),
        out_specs=(spectrum,) * 3,
        check_vma=False,
    )
```

```python
import jax
import jax.numpy as jnp
from jax import lax
from jax.experimental import pallas as pl
from jax.experimental.pallas import tpu as pltpu
from jax.sharding import Mesh, PartitionSpec as P

WAVE = ("yh", "zh", "zl", "x", "c")
PEERS = ("yh", "zl", "x", "lev")
SHARERS = ("zh", "c")
NT = (((1,), (1,)), ((), ()))
NN = (((1,), (0,)), ((), ()))
LIMIT = pltpu.CompilerParams(vmem_limit_bytes=16 * 2**20)


def refined(mesh):
    return Mesh(mesh.devices.reshape(2, 6, 2, 4, 2, 4), WAVE + ("lev",))


def dot(a, b, dims):
    return lax.dot_general(a, b, dims, preferred_element_type=jnp.float32)


def damping_table(level_gain, wavenumbers, total_n):
    scaled = (wavenumbers * (wavenumbers + 1)).astype(jnp.float32) / jnp.float32(
        (total_n - 1) * total_n
    )
    return 1.0 / (1.0 + level_gain[:, None] * scaled[None, :] ** 2)


def pack_matrix(m_ref, o_ref):
    m = m_ref[...].astype(jnp.float32)
    o_ref[0:136, :] = m[:, 0:128].astype(jnp.bfloat16)
    tail = m[:, 128:136]
    flipped = jnp.concatenate([tail, jnp.zeros((120, 8), jnp.float32)], axis=0)
    flipped = jnp.concatenate([flipped, jnp.zeros((256, 120), jnp.float32)], axis=1).T
    o_ref[136:152, :] = jnp.concatenate(
        [flipped[0:8, 0:128], flipped[0:8, 128:256]], axis=0
    ).astype(jnp.bfloat16)


def prepare_kernel(x_hbm, m_hbm, o_hbm, p_ref, x_ref, m_ref, o_ref, sems):
    load_m = pltpu.make_async_copy(m_hbm, m_ref, sems.at[0])
    load_m.start()
    load_x = pltpu.make_async_copy(x_hbm, x_ref, sems.at[1])
    load_x.start()
    load_m.wait()
    pack_matrix(m_ref, p_ref)
    load_x.wait()
    leaving = []
    for h in range(2):
        sides = []
        for c in range(2):
            x = x_ref[:, :, :, h * 384 : h * 384 + 384].astype(jnp.float32)
            rows = jnp.concatenate(
                [x[0, :, c, :], x[1, :, c, :], jnp.zeros((4, 384), jnp.float32)], axis=0
            )
            sides.append(rows.T[:, 0:68])
        both = jnp.stack(sides, axis=1).astype(jnp.bfloat16).reshape(2, 2, 6, 2, 4, 2, 2, 68)
        for l in range(2):
            for yh in range(2):
                for zh in range(6):
                    for zl in range(2):
                        o_ref[yh, zl, :, 2 * h + l, zh] = both[l, yh, zh, zl]
        part = pl.ds(2 * h, 2)
        leave = pltpu.make_async_copy(
            o_ref.at[:, :, :, part], o_hbm.at[:, :, :, part], sems.at[2 + h]
        )
        leave.start()
        leaving.append(leave)
    for leave in leaving:
        leave.wait()


def solve_kernel(x_ref, m_ref, c_ref, o_hbm, stage, sol, o_ref, pairs, sems):
    nz = m_ref.shape[0]
    for z in range(nz):
        parts = ([], [])
        for l in range(4):
            pairs[z * 4 + l, :, 0:68] = x_ref[:, l, z].reshape(32, 68).astype(jnp.float32)
            for c in range(2):
                parts[c].append(pairs[z * 4 + l, pl.ds(c, 16, 2), :])
        x = jnp.concatenate(
            [
                jnp.concatenate(
                    [parts[c][l][:, r * 34 : r * 34 + 34] for l in range(4)], axis=1
                )
                for c in range(2)
                for r in range(2)
            ],
            axis=0,
        ).astype(jnp.bfloat16)
        tail = m_ref[z, 136:152, :]
        x_tail = x[:, 128:136]
        low = dot(x[:, 0:128], m_ref[z, 0:136, :], NT)
        high = jnp.concatenate(
            [dot(x_tail, tail[0:8, :], NN), dot(x_tail, tail[8:16, 0:8], NN)], axis=1
        )
        sol[z * 64 : z * 64 + 64, :] = (low + high).astype(jnp.bfloat16)
    coupled = dot(sol[...], c_ref[...], NT).astype(jnp.bfloat16)
    for z in range(nz):
        both = [
            values[z * 64 : z * 64 + 64, :].astype(jnp.float32) for values in (sol, coupled)
        ]
        for c in range(2):
            for l in range(4):
                stage[l, c, :, z * 136 : z * 136 + 136] = jnp.concatenate(
                    [
                        values[(c * 2 + r) * 16 : (c * 2 + r) * 16 + 16, l * 34 : l * 34 + 34]
                        for values in both
                        for r in range(2)
                    ],
                    axis=1,
                )
    leaving = []
    for l in range(4):
        for t in range(13):
            for c in range(2):
                tile = stage[l, c, :, t * 128 : t * 128 + 128]
                if t == 12:
                    tile = jnp.concatenate(
                        [tile[:, 0:96], jnp.zeros((16, 32), jnp.float32)], axis=1
                    )
                pairs[l * 13 + t, pl.ds(c, 16, 2), :] = tile
            o_ref[:, l, :, t * 128 : t * 128 + 128] = (
                pairs[l * 13 + t].astype(jnp.bfloat16).reshape(16, 2, 128)
            )
        leave = pltpu.make_async_copy(o_ref.at[:, l], o_hbm.at[:, l], sems.at[l])
        leave.start()
        leaving.append(leave)
    for leave in leaving:
        leave.wait()


def place_kernel(q_ref):
    for g in range(3):
        row = lax.broadcasted_iota(jnp.int32, (256, 768), 0)
        col = lax.broadcasted_iota(jnp.int32, (256, 768), 1)
        q, s, l = 4 * g + (row >> 6), (row >> 2) & 15, row & 3
        yh, zl, x = s >> 3, (s >> 2) & 1, s & 3
        place = l * 192 + yh * 96 + (q >> 1) * 16 + zl * 8 + x * 2 + (q & 1)
        q_ref[g * 256 : g * 256 + 256, :] = jnp.where(col == place, 1.0, 0.0).astype(
            jnp.bfloat16
        )


def finish_kernel(
    m_ref, b_ref, heat_ref, q_ref, div_hbm, temp_hbm, stage, div_ref, temp_ref, sems
):
    full = b_ref[...].astype(jnp.float32)
    spans = []
    for c in range(2):
        flipped = full[:, c, :].T
        spans.append([flipped[q * 136 : (q + 1) * 136, :] for q in range(12)])
    total = None
    for g in range(3):
        sides = [jnp.concatenate(spans[c][4 * g : 4 * g + 4], axis=1) for c in range(2)]
        left = jnp.concatenate(sides, axis=0).astype(jnp.bfloat16)
        part = dot(left, q_ref[g * 256 : g * 256 + 256, :], NN)
        total = part if total is None else total + part
    for c in range(2):
        for t in range(6):
            stage[t, pl.ds(c, 136, 2), :] = total[
                c * 136 : (c + 1) * 136, t * 128 : (t + 1) * 128
            ]
    lane = lax.broadcasted_iota(jnp.int32, (2, 768), 1)
    leaving = []
    for r in range(2):
        inside = lane >= m_ref[r]
        for k in range(34):
            at = 2 * (r * 34 + k)
            solved, coupled = (
                jnp.concatenate([stage[t, i : i + 2, :] for t in range(6)], axis=1)
                for i in (at, 136 + at)
            )
            heat = heat_ref[r, k].astype(jnp.float32)
            div_ref[r, k] = jnp.where(inside, solved, 0.0).astype(jnp.bfloat16)
            temp_ref[r, k] = jnp.where(inside, heat - coupled, 0.0).astype(jnp.bfloat16)
        for f, (ready, out) in enumerate(((div_ref, div_hbm), (temp_ref, temp_hbm))):
            leave = pltpu.make_async_copy(ready.at[r], out.at[r], sems.at[2 * r + f])
            leave.start()
            leaving.append(leave)
    for leave in leaving:
        leave.wait()


VMEM = pl.BlockSpec(memory_space=pltpu.VMEM)
SMEM = pl.BlockSpec(memory_space=pltpu.SMEM)
HBM = pl.BlockSpec(memory_space=pltpu.HBM)


def copies(n):
    return pltpu.SemaphoreType.DMA((n,))


def on_device(
    spin_tendency,
    spreading_source,
    heat_source,
    helmholtz_inverses,
    heat_spreading_coupler,
    smoothing_strengths,
    azimuthal_order_list,
):
    rows, parts, lev_local, total_n = spreading_source.shape
    nyh, nzh, nzl, nx, nc = (lax.axis_size(a) for a in WAVE)
    nlev = lax.axis_size("lev")
    peers = nyh * nzl * nx
    shared = nzh * nc
    layers = lev_local * nlev
    zero = jnp.zeros((), jnp.bfloat16)

    def bf16(*shape):
        return jax.ShapeDtypeStruct(shape, jnp.bfloat16)

    def room(*shape, dtype=jnp.bfloat16):
        return pltpu.VMEM(shape, dtype)

    outgoing = (nyh, nzl, nx, nlev, nzh, nc, parts, rows * lev_local)
    sent, packed = pl.pallas_call(
        prepare_kernel,
        out_shape=(bf16(*outgoing), bf16(layers + 16, 128)),
        in_specs=[HBM, HBM],
        out_specs=(HBM, VMEM),
        scratch_shapes=[
            room(rows, lev_local, parts, total_n),
            room(layers, layers),
            room(*outgoing),
            copies(4),
        ],
        compiler_params=LIMIT,
    )(
        pltpu.with_memory_space_constraint(spreading_source.transpose(0, 2, 1, 3), pltpu.HBM),
        pltpu.with_memory_space_constraint(helmholtz_inverses[0, 0], pltpu.HBM),
    )
    sent = sent.reshape(peers * nlev, shared, parts, rows * lev_local)
    got = lax.all_to_all(sent, PEERS, split_axis=0, concat_axis=0, tiled=True)
    matrices = lax.all_gather(packed, SHARERS, axis=0, tiled=False)

    width = 13 * 128
    both = pl.pallas_call(
        solve_kernel,
        out_shape=bf16(peers, nlev, parts, width),
        in_specs=[VMEM] * 3,
        out_specs=HBM,
        scratch_shapes=[
            room(nlev, parts, peers, width, dtype=jnp.float32),
            room(shared * parts * rows * peers, layers),
            room(peers, nlev, parts, width),
            room(nlev * 13, parts * peers, 128, dtype=jnp.float32),
            copies(4),
        ],
        compiler_params=LIMIT,
    )(
        got.reshape(peers, nlev, shared, parts, rows * lev_local),
        matrices,
        heat_spreading_coupler,
    )
    both = both.reshape(peers * nlev, parts, width)
    back = lax.all_to_all(both, PEERS, split_axis=0, concat_axis=0, tiled=True)

    places = pl.pallas_call(
        place_kernel, out_shape=bf16(total_n, total_n), out_specs=VMEM, compiler_params=LIMIT
    )()
    spectrum = (rows, lev_local, parts, total_n)
    divergence, temperature = pl.pallas_call(
        finish_kernel,
        out_shape=(bf16(*spectrum), bf16(*spectrum)),
        in_specs=[SMEM] + [VMEM] * 3,
        out_specs=(HBM, HBM),
        scratch_shapes=[
            room(total_n // 128, 4 * rows * lev_local, 128, dtype=jnp.float32),
            room(*spectrum),
            room(*spectrum),
            copies(4),
        ],
        compiler_params=LIMIT,
    )(azimuthal_order_list, back, heat_source.transpose(0, 2, 1, 3), places)

    level_gain = lax.dynamic_slice_in_dim(
        smoothing_strengths, lax.axis_index("lev") * lev_local, lev_local
    )
    damping = damping_table(level_gain, jnp.arange(total_n, dtype=jnp.int32), total_n)
    spin_updated = (spin_tendency.astype(jnp.float32) * damping[None, None]).astype(jnp.bfloat16)
    interior = (
        jnp.arange(total_n, dtype=jnp.int32)[None, :] >= azimuthal_order_list[:, None]
    )[:, None, None, :]
    return (
        jnp.where(interior, spin_updated, zero),
        divergence.transpose(0, 2, 1, 3),
        temperature.transpose(0, 2, 1, 3),
    )


def solution(mesh):
    spectrum = P(WAVE, None, "lev", None)
    return jax.shard_map(
        on_device,
        mesh=refined(mesh),
        in_specs=(spectrum, spectrum, spectrum, P("lev", WAVE, None, None), P(), P(), P(WAVE)),
        out_specs=(spectrum,) * 3,
        check_vma=False,
    )
```

```python
import jax
import jax.numpy as jnp
from jax import lax
from jax.experimental import pallas as pl
from jax.experimental.pallas import tpu as pltpu
from jax.sharding import Mesh, PartitionSpec as P

WAVE = ("yh", "zh", "zl", "x", "c")
PEERS = ("lev", "x", "zl", "yh")
SHARERS = ("zh", "c")
NT = (((1,), (1,)), ((), ()))
NN = (((1,), (0,)), ((), ()))
LIMIT = pltpu.CompilerParams(vmem_limit_bytes=16 * 2**20)


def refined(mesh):
    return Mesh(mesh.devices.reshape(2, 6, 2, 4, 2, 4), WAVE + ("lev",))


def dot(a, b, dims):
    return lax.dot_general(a, b, dims, preferred_element_type=jnp.float32)


def damping_table(level_gain, wavenumbers, total_n):
    scaled = (wavenumbers * (wavenumbers + 1)).astype(jnp.float32) / jnp.float32(
        (total_n - 1) * total_n
    )
    return 1.0 / (1.0 + level_gain[:, None] * scaled[None, :] ** 2)


def pack_matrix(m_ref, o_ref):
    m = m_ref[...].astype(jnp.float32)
    o_ref[0:136, :] = m[:, 0:128].astype(jnp.bfloat16)
    tail = m[:, 128:136]
    flipped = jnp.concatenate([tail, jnp.zeros((120, 8), jnp.float32)], axis=0)
    flipped = jnp.concatenate([flipped, jnp.zeros((256, 120), jnp.float32)], axis=1).T
    o_ref[136:152, :] = jnp.concatenate(
        [flipped[0:8, 0:128], flipped[0:8, 128:256]], axis=0
    ).astype(jnp.bfloat16)


def prepare_kernel(x_hbm, m_hbm, o_hbm, p_ref, x_ref, m_ref, o_ref, sems):
    load_m = pltpu.make_async_copy(m_hbm, m_ref, sems.at[0])
    load_m.start()
    load_x = pltpu.make_async_copy(x_hbm, x_ref, sems.at[1])
    load_x.start()
    load_m.wait()
    pack_matrix(m_ref, p_ref)
    load_x.wait()
    leaving = []
    for h in range(2):
        sides = []
        for c in range(2):
            x = x_ref[:, :, :, h * 384 : h * 384 + 384].astype(jnp.float32)
            rows = jnp.concatenate(
                [x[0, :, c, :], x[1, :, c, :], jnp.zeros((4, 384), jnp.float32)], axis=0
            )
            sides.append(rows.T[:, 0:68])
        both = jnp.stack(sides, axis=1).astype(jnp.bfloat16).reshape(2, 2, 6, 2, 4, 2, 2, 68)
        for l in range(2):
            for yh in range(2):
                for zh in range(6):
                    for zl in range(2):
                        o_ref[2 * h + l, :, zl, yh, zh] = both[l, yh, zh, zl]
        part = pl.ds(2 * h, 2)
        leave = pltpu.make_async_copy(
            o_ref.at[part], o_hbm.at[part], sems.at[2 + h]
        )
        leave.start()
        leaving.append(leave)
    for leave in leaving:
        leave.wait()


def solve_kernel(x_ref, m_ref, c_ref, o_hbm, stage, sol, o_ref, pairs, sems):
    nz = m_ref.shape[0]
    for z in range(nz):
        parts = ([], [])
        for l in range(4):
            pairs[z * 4 + l, :, 0:68] = x_ref[l, :, z].reshape(32, 68).astype(jnp.float32)
            for c in range(2):
                parts[c].append(pairs[z * 4 + l, pl.ds(c, 16, 2), :])
        x = jnp.concatenate(
            [
                jnp.concatenate(
                    [parts[c][l][:, r * 34 : r * 34 + 34] for l in range(4)], axis=1
                )
                for c in range(2)
                for r in range(2)
            ],
            axis=0,
        ).astype(jnp.bfloat16)
        tail = m_ref[z, 136:152, :]
        x_tail = x[:, 128:136]
        low = dot(x[:, 0:128], m_ref[z, 0:136, :], NT)
        high = jnp.concatenate(
            [dot(x_tail, tail[0:8, :], NN), dot(x_tail, tail[8:16, 0:8], NN)], axis=1
        )
        sol[z * 64 : z * 64 + 64, :] = (low + high).astype(jnp.bfloat16)
    coupled = dot(sol[...], c_ref[...], NT).astype(jnp.bfloat16)
    for z in range(nz):
        both = [
            values[z * 64 : z * 64 + 64, :].astype(jnp.float32) for values in (sol, coupled)
        ]
        for c in range(2):
            for l in range(4):
                stage[l, c, :, z * 136 : z * 136 + 136] = jnp.concatenate(
                    [
                        values[(c * 2 + r) * 16 : (c * 2 + r) * 16 + 16, l * 34 : l * 34 + 34]
                        for values in both
                        for r in range(2)
                    ],
                    axis=1,
                )
    leaving = []
    for l in range(4):
        for t in range(13):
            for c in range(2):
                tile = stage[l, c, :, t * 128 : t * 128 + 128]
                if t == 12:
                    tile = jnp.concatenate(
                        [tile[:, 0:96], jnp.zeros((16, 32), jnp.float32)], axis=1
                    )
                pairs[l * 13 + t, pl.ds(c, 16, 2), :] = tile
            o_ref[l, :, :, t * 128 : t * 128 + 128] = (
                pairs[l * 13 + t].astype(jnp.bfloat16).reshape(16, 2, 128)
            )
        leave = pltpu.make_async_copy(o_ref.at[l], o_hbm.at[l], sems.at[l])
        leave.start()
        leaving.append(leave)
    for leave in leaving:
        leave.wait()


def place_kernel(q_ref):
    for g in range(3):
        row = lax.broadcasted_iota(jnp.int32, (256, 768), 0)
        col = lax.broadcasted_iota(jnp.int32, (256, 768), 1)
        q, l = 4 * g + (row >> 6), (row >> 4) & 3
        x, zl, yh = (row >> 2) & 3, (row >> 1) & 1, row & 1
        place = l * 192 + yh * 96 + (q >> 1) * 16 + zl * 8 + x * 2 + (q & 1)
        q_ref[g * 256 : g * 256 + 256, :] = jnp.where(col == place, 1.0, 0.0).astype(
            jnp.bfloat16
        )


def finish_kernel(
    m_ref, b_ref, heat_ref, q_ref, div_hbm, temp_hbm, stage, div_ref, temp_ref, sems
):
    full = b_ref[...].astype(jnp.float32)
    spans = []
    for c in range(2):
        flipped = full[:, c, :].T
        spans.append([flipped[q * 136 : (q + 1) * 136, :] for q in range(12)])
    total = None
    for g in range(3):
        sides = [jnp.concatenate(spans[c][4 * g : 4 * g + 4], axis=1) for c in range(2)]
        left = jnp.concatenate(sides, axis=0).astype(jnp.bfloat16)
        part = dot(left, q_ref[g * 256 : g * 256 + 256, :], NN)
        total = part if total is None else total + part
    for c in range(2):
        for t in range(6):
            stage[t, pl.ds(c, 136, 2), :] = total[
                c * 136 : (c + 1) * 136, t * 128 : (t + 1) * 128
            ]
    lane = lax.broadcasted_iota(jnp.int32, (2, 768), 1)
    leaving = []
    for r in range(2):
        inside = lane >= m_ref[r]
        for k in range(34):
            at = 2 * (r * 34 + k)
            solved, coupled = (
                jnp.concatenate([stage[t, i : i + 2, :] for t in range(6)], axis=1)
                for i in (at, 136 + at)
            )
            heat = heat_ref[r, k].astype(jnp.float32)
            div_ref[r, k] = jnp.where(inside, solved, 0.0).astype(jnp.bfloat16)
            temp_ref[r, k] = jnp.where(inside, heat - coupled, 0.0).astype(jnp.bfloat16)
        for f, (ready, out) in enumerate(((div_ref, div_hbm), (temp_ref, temp_hbm))):
            leave = pltpu.make_async_copy(ready.at[r], out.at[r], sems.at[2 * r + f])
            leave.start()
            leaving.append(leave)
    for leave in leaving:
        leave.wait()


VMEM = pl.BlockSpec(memory_space=pltpu.VMEM)
SMEM = pl.BlockSpec(memory_space=pltpu.SMEM)
HBM = pl.BlockSpec(memory_space=pltpu.HBM)


def copies(n):
    return pltpu.SemaphoreType.DMA((n,))


def on_device(
    spin_tendency,
    spreading_source,
    heat_source,
    helmholtz_inverses,
    heat_spreading_coupler,
    smoothing_strengths,
    azimuthal_order_list,
):
    rows, parts, lev_local, total_n = spreading_source.shape
    nyh, nzh, nzl, nx, nc = (lax.axis_size(a) for a in WAVE)
    nlev = lax.axis_size("lev")
    peers = nyh * nzl * nx
    shared = nzh * nc
    layers = lev_local * nlev
    zero = jnp.zeros((), jnp.bfloat16)

    def bf16(*shape):
        return jax.ShapeDtypeStruct(shape, jnp.bfloat16)

    def room(*shape, dtype=jnp.bfloat16):
        return pltpu.VMEM(shape, dtype)

    outgoing = (nlev, nx, nzl, nyh, nzh, nc, parts, rows * lev_local)
    sent, packed = pl.pallas_call(
        prepare_kernel,
        out_shape=(bf16(*outgoing), bf16(layers + 16, 128)),
        in_specs=[HBM, HBM],
        out_specs=(HBM, VMEM),
        scratch_shapes=[
            room(rows, lev_local, parts, total_n),
            room(layers, layers),
            room(*outgoing),
            copies(4),
        ],
        compiler_params=LIMIT,
    )(
        pltpu.with_memory_space_constraint(spreading_source.transpose(0, 2, 1, 3), pltpu.HBM),
        pltpu.with_memory_space_constraint(helmholtz_inverses[0, 0], pltpu.HBM),
    )
    sent = sent.reshape(peers * nlev, shared, parts, rows * lev_local)
    got = lax.all_to_all(sent, PEERS, split_axis=0, concat_axis=0, tiled=True)
    matrices = lax.all_gather(packed, SHARERS, axis=0, tiled=False)

    width = 13 * 128
    both = pl.pallas_call(
        solve_kernel,
        out_shape=bf16(nlev, peers, parts, width),
        in_specs=[VMEM] * 3,
        out_specs=HBM,
        scratch_shapes=[
            room(nlev, parts, peers, width, dtype=jnp.float32),
            room(shared * parts * rows * peers, layers),
            room(nlev, peers, parts, width),
            room(nlev * 13, parts * peers, 128, dtype=jnp.float32),
            copies(4),
        ],
        compiler_params=LIMIT,
    )(
        got.reshape(nlev, peers, shared, parts, rows * lev_local),
        matrices,
        heat_spreading_coupler,
    )
    both = both.reshape(peers * nlev, parts, width)
    back = lax.all_to_all(both, PEERS, split_axis=0, concat_axis=0, tiled=True)

    places = pl.pallas_call(
        place_kernel, out_shape=bf16(total_n, total_n), out_specs=VMEM, compiler_params=LIMIT
    )()
    spectrum = (rows, lev_local, parts, total_n)
    divergence, temperature = pl.pallas_call(
        finish_kernel,
        out_shape=(bf16(*spectrum), bf16(*spectrum)),
        in_specs=[SMEM] + [VMEM] * 3,
        out_specs=(HBM, HBM),
        scratch_shapes=[
            room(total_n // 128, 4 * rows * lev_local, 128, dtype=jnp.float32),
            room(*spectrum),
            room(*spectrum),
            copies(4),
        ],
        compiler_params=LIMIT,
    )(azimuthal_order_list, back, heat_source.transpose(0, 2, 1, 3), places)

    level_gain = lax.dynamic_slice_in_dim(
        smoothing_strengths, lax.axis_index("lev") * lev_local, lev_local
    )
    damping = damping_table(level_gain, jnp.arange(total_n, dtype=jnp.int32), total_n)
    spin_updated = (spin_tendency.astype(jnp.float32) * damping[None, None]).astype(jnp.bfloat16)
    interior = (
        jnp.arange(total_n, dtype=jnp.int32)[None, :] >= azimuthal_order_list[:, None]
    )[:, None, None, :]
    return (
        jnp.where(interior, spin_updated, zero),
        divergence.transpose(0, 2, 1, 3),
        temperature.transpose(0, 2, 1, 3),
    )


def solution(mesh):
    spectrum = P(WAVE, None, "lev", None)
    return jax.shard_map(
        on_device,
        mesh=refined(mesh),
        in_specs=(spectrum, spectrum, spectrum, P("lev", WAVE, None, None), P(), P(), P(WAVE)),
        out_specs=(spectrum,) * 3,
        check_vma=False,
    )
```

```python
import jax
import jax.numpy as jnp
from jax import lax
from jax.experimental import pallas as pl
from jax.experimental.pallas import tpu as pltpu
from jax.sharding import Mesh, PartitionSpec as P

WAVE = ("yh", "zh", "zl", "x", "c")
PEERS = ("zl", "x", "yh", "lev")
SHARERS = ("zh", "c")
NT = (((1,), (1,)), ((), ()))
NN = (((1,), (0,)), ((), ()))
LIMIT = pltpu.CompilerParams(vmem_limit_bytes=16 * 2**20)


def refined(mesh):
    return Mesh(mesh.devices.reshape(2, 6, 2, 4, 2, 4), WAVE + ("lev",))


def dot(a, b, dims):
    return lax.dot_general(a, b, dims, preferred_element_type=jnp.float32)


def damping_table(level_gain, wavenumbers, total_n):
    scaled = (wavenumbers * (wavenumbers + 1)).astype(jnp.float32) / jnp.float32(
        (total_n - 1) * total_n
    )
    return 1.0 / (1.0 + level_gain[:, None] * scaled[None, :] ** 2)


def pack_matrix(m_ref, o_ref):
    m = m_ref[...].astype(jnp.float32)
    o_ref[0:136, :] = m[:, 0:128].astype(jnp.bfloat16)
    tail = m[:, 128:136]
    flipped = jnp.concatenate([tail, jnp.zeros((120, 8), jnp.float32)], axis=0)
    flipped = jnp.concatenate([flipped, jnp.zeros((256, 120), jnp.float32)], axis=1).T
    o_ref[136:152, :] = jnp.concatenate(
        [flipped[0:8, 0:128], flipped[0:8, 128:256]], axis=0
    ).astype(jnp.bfloat16)


def prepare_kernel(x_hbm, m_hbm, o_hbm, p_ref, x_ref, m_ref, o_ref, sems):
    load_m = pltpu.make_async_copy(m_hbm, m_ref, sems.at[0])
    load_m.start()
    load_x = pltpu.make_async_copy(x_hbm, x_ref, sems.at[1])
    load_x.start()
    load_m.wait()
    pack_matrix(m_ref, p_ref)
    load_x.wait()
    leaving = []
    for h in range(2):
        sides = []
        for c in range(2):
            x = x_ref[:, :, :, h * 384 : h * 384 + 384].astype(jnp.float32)
            rows = jnp.concatenate(
                [x[0, :, c, :], x[1, :, c, :], jnp.zeros((4, 384), jnp.float32)], axis=0
            )
            sides.append(rows.T[:, 0:68])
        both = jnp.stack(sides, axis=1).astype(jnp.bfloat16).reshape(2, 2, 6, 2, 4, 2, 2, 68)
        for l in range(2):
            for yh in range(2):
                for zh in range(6):
                    for zl in range(2):
                        o_ref[zl, :, yh, 2 * h + l, zh] = both[l, yh, zh, zl]
        part = pl.ds(2 * h, 2)
        leave = pltpu.make_async_copy(
            o_ref.at[:, :, :, part], o_hbm.at[:, :, :, part], sems.at[2 + h]
        )
        leave.start()
        leaving.append(leave)
    for leave in leaving:
        leave.wait()


def solve_kernel(x_ref, m_ref, c_ref, o_hbm, stage, sol, o_ref, pairs, sems):
    nz = m_ref.shape[0]
    for z in range(nz):
        parts = ([], [])
        for l in range(4):
            pairs[z * 4 + l, :, 0:68] = x_ref[:, l, z].reshape(32, 68).astype(jnp.float32)
            for c in range(2):
                parts[c].append(pairs[z * 4 + l, pl.ds(c, 16, 2), :])
        x = jnp.concatenate(
            [
                jnp.concatenate(
                    [parts[c][l][:, r * 34 : r * 34 + 34] for l in range(4)], axis=1
                )
                for c in range(2)
                for r in range(2)
            ],
            axis=0,
        ).astype(jnp.bfloat16)
        tail = m_ref[z, 136:152, :]
        x_tail = x[:, 128:136]
        low = dot(x[:, 0:128], m_ref[z, 0:136, :], NT)
        high = jnp.concatenate(
            [dot(x_tail, tail[0:8, :], NN), dot(x_tail, tail[8:16, 0:8], NN)], axis=1
        )
        sol[z * 64 : z * 64 + 64, :] = (low + high).astype(jnp.bfloat16)
    coupled = dot(sol[...], c_ref[...], NT).astype(jnp.bfloat16)
    for z in range(nz):
        both = [
            values[z * 64 : z * 64 + 64, :].astype(jnp.float32) for values in (sol, coupled)
        ]
        for c in range(2):
            for l in range(4):
                stage[l, c, :, z * 136 : z * 136 + 136] = jnp.concatenate(
                    [
                        values[(c * 2 + r) * 16 : (c * 2 + r) * 16 + 16, l * 34 : l * 34 + 34]
                        for values in both
                        for r in range(2)
                    ],
                    axis=1,
                )
    leaving = []
    for l in range(4):
        for t in range(13):
            for c in range(2):
                tile = stage[l, c, :, t * 128 : t * 128 + 128]
                if t == 12:
                    tile = jnp.concatenate(
                        [tile[:, 0:96], jnp.zeros((16, 32), jnp.float32)], axis=1
                    )
                pairs[l * 13 + t, pl.ds(c, 16, 2), :] = tile
            o_ref[:, l, :, t * 128 : t * 128 + 128] = (
                pairs[l * 13 + t].astype(jnp.bfloat16).reshape(16, 2, 128)
            )
        leave = pltpu.make_async_copy(o_ref.at[:, l], o_hbm.at[:, l], sems.at[l])
        leave.start()
        leaving.append(leave)
    for leave in leaving:
        leave.wait()


def place_kernel(q_ref):
    for g in range(3):
        row = lax.broadcasted_iota(jnp.int32, (256, 768), 0)
        col = lax.broadcasted_iota(jnp.int32, (256, 768), 1)
        q, s, l = 4 * g + (row >> 6), (row >> 2) & 15, row & 3
        zl, x, yh = s >> 3, (s >> 1) & 3, s & 1
        place = l * 192 + yh * 96 + (q >> 1) * 16 + zl * 8 + x * 2 + (q & 1)
        q_ref[g * 256 : g * 256 + 256, :] = jnp.where(col == place, 1.0, 0.0).astype(
            jnp.bfloat16
        )


def finish_kernel(
    m_ref, b_ref, heat_ref, q_ref, div_hbm, temp_hbm, stage, div_ref, temp_ref, sems
):
    full = b_ref[...].astype(jnp.float32)
    spans = []
    for c in range(2):
        flipped = full[:, c, :].T
        spans.append([flipped[q * 136 : (q + 1) * 136, :] for q in range(12)])
    total = None
    for g in range(3):
        sides = [jnp.concatenate(spans[c][4 * g : 4 * g + 4], axis=1) for c in range(2)]
        left = jnp.concatenate(sides, axis=0).astype(jnp.bfloat16)
        part = dot(left, q_ref[g * 256 : g * 256 + 256, :], NN)
        total = part if total is None else total + part
    for c in range(2):
        for t in range(6):
            stage[t, pl.ds(c, 136, 2), :] = total[
                c * 136 : (c + 1) * 136, t * 128 : (t + 1) * 128
            ]
    lane = lax.broadcasted_iota(jnp.int32, (2, 768), 1)
    leaving = []
    for r in range(2):
        inside = lane >= m_ref[r]
        for k in range(34):
            at = 2 * (r * 34 + k)
            solved, coupled = (
                jnp.concatenate([stage[t, i : i + 2, :] for t in range(6)], axis=1)
                for i in (at, 136 + at)
            )
            heat = heat_ref[r, k].astype(jnp.float32)
            div_ref[r, k] = jnp.where(inside, solved, 0.0).astype(jnp.bfloat16)
            temp_ref[r, k] = jnp.where(inside, heat - coupled, 0.0).astype(jnp.bfloat16)
        for f, (ready, out) in enumerate(((div_ref, div_hbm), (temp_ref, temp_hbm))):
            leave = pltpu.make_async_copy(ready.at[r], out.at[r], sems.at[2 * r + f])
            leave.start()
            leaving.append(leave)
    for leave in leaving:
        leave.wait()


VMEM = pl.BlockSpec(memory_space=pltpu.VMEM)
SMEM = pl.BlockSpec(memory_space=pltpu.SMEM)
HBM = pl.BlockSpec(memory_space=pltpu.HBM)


def copies(n):
    return pltpu.SemaphoreType.DMA((n,))


def on_device(
    spin_tendency,
    spreading_source,
    heat_source,
    helmholtz_inverses,
    heat_spreading_coupler,
    smoothing_strengths,
    azimuthal_order_list,
):
    rows, parts, lev_local, total_n = spreading_source.shape
    nyh, nzh, nzl, nx, nc = (lax.axis_size(a) for a in WAVE)
    nlev = lax.axis_size("lev")
    peers = nyh * nzl * nx
    shared = nzh * nc
    layers = lev_local * nlev
    zero = jnp.zeros((), jnp.bfloat16)

    def bf16(*shape):
        return jax.ShapeDtypeStruct(shape, jnp.bfloat16)

    def room(*shape, dtype=jnp.bfloat16):
        return pltpu.VMEM(shape, dtype)

    outgoing = (nzl, nx, nyh, nlev, nzh, nc, parts, rows * lev_local)
    sent, packed = pl.pallas_call(
        prepare_kernel,
        out_shape=(bf16(*outgoing), bf16(layers + 16, 128)),
        in_specs=[HBM, HBM],
        out_specs=(HBM, VMEM),
        scratch_shapes=[
            room(rows, lev_local, parts, total_n),
            room(layers, layers),
            room(*outgoing),
            copies(4),
        ],
        compiler_params=LIMIT,
    )(
        pltpu.with_memory_space_constraint(spreading_source.transpose(0, 2, 1, 3), pltpu.HBM),
        pltpu.with_memory_space_constraint(helmholtz_inverses[0, 0], pltpu.HBM),
    )
    sent = sent.reshape(peers * nlev, shared, parts, rows * lev_local)
    got = lax.all_to_all(sent, PEERS, split_axis=0, concat_axis=0, tiled=True)
    matrices = lax.all_gather(packed, SHARERS, axis=0, tiled=False)

    width = 13 * 128
    both = pl.pallas_call(
        solve_kernel,
        out_shape=bf16(peers, nlev, parts, width),
        in_specs=[VMEM] * 3,
        out_specs=HBM,
        scratch_shapes=[
            room(nlev, parts, peers, width, dtype=jnp.float32),
            room(shared * parts * rows * peers, layers),
            room(peers, nlev, parts, width),
            room(nlev * 13, parts * peers, 128, dtype=jnp.float32),
            copies(4),
        ],
        compiler_params=LIMIT,
    )(
        got.reshape(peers, nlev, shared, parts, rows * lev_local),
        matrices,
        heat_spreading_coupler,
    )
    both = both.reshape(peers * nlev, parts, width)
    back = lax.all_to_all(both, PEERS, split_axis=0, concat_axis=0, tiled=True)

    places = pl.pallas_call(
        place_kernel, out_shape=bf16(total_n, total_n), out_specs=VMEM, compiler_params=LIMIT
    )()
    spectrum = (rows, lev_local, parts, total_n)
    divergence, temperature = pl.pallas_call(
        finish_kernel,
        out_shape=(bf16(*spectrum), bf16(*spectrum)),
        in_specs=[SMEM] + [VMEM] * 3,
        out_specs=(HBM, HBM),
        scratch_shapes=[
            room(total_n // 128, 4 * rows * lev_local, 128, dtype=jnp.float32),
            room(*spectrum),
            room(*spectrum),
            copies(4),
        ],
        compiler_params=LIMIT,
    )(azimuthal_order_list, back, heat_source.transpose(0, 2, 1, 3), places)

    level_gain = lax.dynamic_slice_in_dim(
        smoothing_strengths, lax.axis_index("lev") * lev_local, lev_local
    )
    damping = damping_table(level_gain, jnp.arange(total_n, dtype=jnp.int32), total_n)
    spin_updated = (spin_tendency.astype(jnp.float32) * damping[None, None]).astype(jnp.bfloat16)
    interior = (
        jnp.arange(total_n, dtype=jnp.int32)[None, :] >= azimuthal_order_list[:, None]
    )[:, None, None, :]
    return (
        jnp.where(interior, spin_updated, zero),
        divergence.transpose(0, 2, 1, 3),
        temperature.transpose(0, 2, 1, 3),
    )


def solution(mesh):
    spectrum = P(WAVE, None, "lev", None)
    return jax.shard_map(
        on_device,
        mesh=refined(mesh),
        in_specs=(spectrum, spectrum, spectrum, P("lev", WAVE, None, None), P(), P(), P(WAVE)),
        out_specs=(spectrum,) * 3,
        check_vma=False,
    )
```

```python
import jax
import jax.numpy as jnp
from jax import lax
from jax.experimental import pallas as pl
from jax.experimental.pallas import tpu as pltpu
from jax.sharding import Mesh, PartitionSpec as P

WAVE = ("yh", "zh", "zl", "x", "c")
PEERS = ("yh", "zl", "lev", "x")
SHARERS = ("zh", "c")
NT = (((1,), (1,)), ((), ()))
NN = (((1,), (0,)), ((), ()))
LIMIT = pltpu.CompilerParams(vmem_limit_bytes=16 * 2**20)


def refined(mesh):
    return Mesh(mesh.devices.reshape(2, 6, 2, 4, 2, 4), WAVE + ("lev",))


def dot(a, b, dims):
    return lax.dot_general(a, b, dims, preferred_element_type=jnp.float32)


def damping_table(level_gain, wavenumbers, total_n):
    scaled = (wavenumbers * (wavenumbers + 1)).astype(jnp.float32) / jnp.float32(
        (total_n - 1) * total_n
    )
    return 1.0 / (1.0 + level_gain[:, None] * scaled[None, :] ** 2)


def pack_matrix(m_ref, o_ref):
    m = m_ref[...].astype(jnp.float32)
    o_ref[0:136, :] = m[:, 0:128].astype(jnp.bfloat16)
    tail = m[:, 128:136]
    flipped = jnp.concatenate([tail, jnp.zeros((120, 8), jnp.float32)], axis=0)
    flipped = jnp.concatenate([flipped, jnp.zeros((256, 120), jnp.float32)], axis=1).T
    o_ref[136:152, :] = jnp.concatenate(
        [flipped[0:8, 0:128], flipped[0:8, 128:256]], axis=0
    ).astype(jnp.bfloat16)


def prepare_kernel(x_hbm, m_hbm, o_hbm, p_ref, x_ref, m_ref, o_ref, sems):
    load_m = pltpu.make_async_copy(m_hbm, m_ref, sems.at[0])
    load_m.start()
    load_x = pltpu.make_async_copy(x_hbm, x_ref, sems.at[1])
    load_x.start()
    load_m.wait()
    pack_matrix(m_ref, p_ref)
    load_x.wait()
    leaving = []
    for h in range(2):
        sides = []
        for c in range(2):
            x = x_ref[:, :, :, h * 384 : h * 384 + 384].astype(jnp.float32)
            rows = jnp.concatenate(
                [x[0, :, c, :], x[1, :, c, :], jnp.zeros((4, 384), jnp.float32)], axis=0
            )
            sides.append(rows.T[:, 0:68])
        both = jnp.stack(sides, axis=1).astype(jnp.bfloat16).reshape(2, 2, 6, 2, 4, 2, 2, 68)
        for l in range(2):
            for yh in range(2):
                for zh in range(6):
                    for zl in range(2):
                        o_ref[yh, zl, 2 * h + l, :, zh] = both[l, yh, zh, zl]
        part = pl.ds(2 * h, 2)
        leave = pltpu.make_async_copy(
            o_ref.at[:, :, part], o_hbm.at[:, :, part], sems.at[2 + h]
        )
        leave.start()
        leaving.append(leave)
    for leave in leaving:
        leave.wait()


def solve_kernel(x_ref, m_ref, c_ref, o_hbm, stage, sol, o_ref, pairs, sems):
    nz = m_ref.shape[0]
    for z in range(nz):
        parts = ([], [])
        for l in range(4):
            pairs[z * 4 + l, :, 0:68] = x_ref[:, l, :, z].reshape(32, 68).astype(jnp.float32)
            for c in range(2):
                parts[c].append(pairs[z * 4 + l, pl.ds(c, 16, 2), :])
        x = jnp.concatenate(
            [
                jnp.concatenate(
                    [parts[c][l][:, r * 34 : r * 34 + 34] for l in range(4)], axis=1
                )
                for c in range(2)
                for r in range(2)
            ],
            axis=0,
        ).astype(jnp.bfloat16)
        tail = m_ref[z, 136:152, :]
        x_tail = x[:, 128:136]
        low = dot(x[:, 0:128], m_ref[z, 0:136, :], NT)
        high = jnp.concatenate(
            [dot(x_tail, tail[0:8, :], NN), dot(x_tail, tail[8:16, 0:8], NN)], axis=1
        )
        sol[z * 64 : z * 64 + 64, :] = (low + high).astype(jnp.bfloat16)
    coupled = dot(sol[...], c_ref[...], NT).astype(jnp.bfloat16)
    for z in range(nz):
        both = [
            values[z * 64 : z * 64 + 64, :].astype(jnp.float32) for values in (sol, coupled)
        ]
        for c in range(2):
            for l in range(4):
                stage[l, c, :, z * 136 : z * 136 + 136] = jnp.concatenate(
                    [
                        values[(c * 2 + r) * 16 : (c * 2 + r) * 16 + 16, l * 34 : l * 34 + 34]
                        for values in both
                        for r in range(2)
                    ],
                    axis=1,
                )
    leaving = []
    for l in range(4):
        for t in range(13):
            for c in range(2):
                tile = stage[l, c, :, t * 128 : t * 128 + 128]
                if t == 12:
                    tile = jnp.concatenate(
                        [tile[:, 0:96], jnp.zeros((16, 32), jnp.float32)], axis=1
                    )
                pairs[l * 13 + t, pl.ds(c, 16, 2), :] = tile
            o_ref[:, l, :, :, t * 128 : t * 128 + 128] = (
                pairs[l * 13 + t].astype(jnp.bfloat16).reshape(4, 4, 2, 128)
            )
        leave = pltpu.make_async_copy(o_ref.at[:, l], o_hbm.at[:, l], sems.at[l])
        leave.start()
        leaving.append(leave)
    for leave in leaving:
        leave.wait()


def place_kernel(q_ref):
    for g in range(3):
        row = lax.broadcasted_iota(jnp.int32, (256, 768), 0)
        col = lax.broadcasted_iota(jnp.int32, (256, 768), 1)
        q, l = 4 * g + (row >> 6), (row >> 2) & 3
        yh, zl, x = (row >> 5) & 1, (row >> 4) & 1, row & 3
        place = l * 192 + yh * 96 + (q >> 1) * 16 + zl * 8 + x * 2 + (q & 1)
        q_ref[g * 256 : g * 256 + 256, :] = jnp.where(col == place, 1.0, 0.0).astype(
            jnp.bfloat16
        )


def finish_kernel(
    m_ref, b_ref, heat_ref, q_ref, div_hbm, temp_hbm, stage, div_ref, temp_ref, sems
):
    full = b_ref[...].astype(jnp.float32)
    spans = []
    for c in range(2):
        flipped = full[:, c, :].T
        spans.append([flipped[q * 136 : (q + 1) * 136, :] for q in range(12)])
    total = None
    for g in range(3):
        sides = [jnp.concatenate(spans[c][4 * g : 4 * g + 4], axis=1) for c in range(2)]
        left = jnp.concatenate(sides, axis=0).astype(jnp.bfloat16)
        part = dot(left, q_ref[g * 256 : g * 256 + 256, :], NN)
        total = part if total is None else total + part
    for c in range(2):
        for t in range(6):
            stage[t, pl.ds(c, 136, 2), :] = total[
                c * 136 : (c + 1) * 136, t * 128 : (t + 1) * 128
            ]
    lane = lax.broadcasted_iota(jnp.int32, (2, 768), 1)
    leaving = []
    for r in range(2):
        inside = lane >= m_ref[r]
        for k in range(34):
            at = 2 * (r * 34 + k)
            solved, coupled = (
                jnp.concatenate([stage[t, i : i + 2, :] for t in range(6)], axis=1)
                for i in (at, 136 + at)
            )
            heat = heat_ref[r, k].astype(jnp.float32)
            div_ref[r, k] = jnp.where(inside, solved, 0.0).astype(jnp.bfloat16)
            temp_ref[r, k] = jnp.where(inside, heat - coupled, 0.0).astype(jnp.bfloat16)
        for f, (ready, out) in enumerate(((div_ref, div_hbm), (temp_ref, temp_hbm))):
            leave = pltpu.make_async_copy(ready.at[r], out.at[r], sems.at[2 * r + f])
            leave.start()
            leaving.append(leave)
    for leave in leaving:
        leave.wait()


VMEM = pl.BlockSpec(memory_space=pltpu.VMEM)
SMEM = pl.BlockSpec(memory_space=pltpu.SMEM)
HBM = pl.BlockSpec(memory_space=pltpu.HBM)


def copies(n):
    return pltpu.SemaphoreType.DMA((n,))


def on_device(
    spin_tendency,
    spreading_source,
    heat_source,
    helmholtz_inverses,
    heat_spreading_coupler,
    smoothing_strengths,
    azimuthal_order_list,
):
    rows, parts, lev_local, total_n = spreading_source.shape
    nyh, nzh, nzl, nx, nc = (lax.axis_size(a) for a in WAVE)
    nlev = lax.axis_size("lev")
    peers = nyh * nzl * nx
    shared = nzh * nc
    layers = lev_local * nlev
    zero = jnp.zeros((), jnp.bfloat16)

    def bf16(*shape):
        return jax.ShapeDtypeStruct(shape, jnp.bfloat16)

    def room(*shape, dtype=jnp.bfloat16):
        return pltpu.VMEM(shape, dtype)

    outgoing = (nyh, nzl, nlev, nx, nzh, nc, parts, rows * lev_local)
    sent, packed = pl.pallas_call(
        prepare_kernel,
        out_shape=(bf16(*outgoing), bf16(layers + 16, 128)),
        in_specs=[HBM, HBM],
        out_specs=(HBM, VMEM),
        scratch_shapes=[
            room(rows, lev_local, parts, total_n),
            room(layers, layers),
            room(*outgoing),
            copies(4),
        ],
        compiler_params=LIMIT,
    )(
        pltpu.with_memory_space_constraint(spreading_source.transpose(0, 2, 1, 3), pltpu.HBM),
        pltpu.with_memory_space_constraint(helmholtz_inverses[0, 0], pltpu.HBM),
    )
    sent = sent.reshape(peers * nlev, shared, parts, rows * lev_local)
    got = lax.all_to_all(sent, PEERS, split_axis=0, concat_axis=0, tiled=True)
    matrices = lax.all_gather(packed, SHARERS, axis=0, tiled=False)

    width = 13 * 128
    both = pl.pallas_call(
        solve_kernel,
        out_shape=bf16(nyh * nzl, nlev, nx, parts, width),
        in_specs=[VMEM] * 3,
        out_specs=HBM,
        scratch_shapes=[
            room(nlev, parts, peers, width, dtype=jnp.float32),
            room(shared * parts * rows * peers, layers),
            room(nyh * nzl, nlev, nx, parts, width),
            room(nlev * 13, parts * peers, 128, dtype=jnp.float32),
            copies(4),
        ],
        compiler_params=LIMIT,
    )(
        got.reshape(nyh * nzl, nlev, nx, shared, parts, rows * lev_local),
        matrices,
        heat_spreading_coupler,
    )
    both = both.reshape(peers * nlev, parts, width)
    back = lax.all_to_all(both, PEERS, split_axis=0, concat_axis=0, tiled=True)

    places = pl.pallas_call(
        place_kernel, out_shape=bf16(total_n, total_n), out_specs=VMEM, compiler_params=LIMIT
    )()
    spectrum = (rows, lev_local, parts, total_n)
    divergence, temperature = pl.pallas_call(
        finish_kernel,
        out_shape=(bf16(*spectrum), bf16(*spectrum)),
        in_specs=[SMEM] + [VMEM] * 3,
        out_specs=(HBM, HBM),
        scratch_shapes=[
            room(total_n // 128, 4 * rows * lev_local, 128, dtype=jnp.float32),
            room(*spectrum),
            room(*spectrum),
            copies(4),
        ],
        compiler_params=LIMIT,
    )(azimuthal_order_list, back, heat_source.transpose(0, 2, 1, 3), places)

    level_gain = lax.dynamic_slice_in_dim(
        smoothing_strengths, lax.axis_index("lev") * lev_local, lev_local
    )
    damping = damping_table(level_gain, jnp.arange(total_n, dtype=jnp.int32), total_n)
    spin_updated = (spin_tendency.astype(jnp.float32) * damping[None, None]).astype(jnp.bfloat16)
    interior = (
        jnp.arange(total_n, dtype=jnp.int32)[None, :] >= azimuthal_order_list[:, None]
    )[:, None, None, :]
    return (
        jnp.where(interior, spin_updated, zero),
        divergence.transpose(0, 2, 1, 3),
        temperature.transpose(0, 2, 1, 3),
    )


def solution(mesh):
    spectrum = P(WAVE, None, "lev", None)
    return jax.shard_map(
        on_device,
        mesh=refined(mesh),
        in_specs=(spectrum, spectrum, spectrum, P("lev", WAVE, None, None), P(), P(), P(WAVE)),
        out_specs=(spectrum,) * 3,
        check_vma=False,
    )
```

```python
import jax
import jax.numpy as jnp
from jax import lax
from jax.experimental import pallas as pl
from jax.experimental.pallas import tpu as pltpu
from jax.sharding import Mesh, PartitionSpec as P

WAVE = ("yh", "zh", "zl", "x", "c")
PEERS = ("yh", "zl", "x", "lev")
SHARERS = ("zh", "c")
NT = (((1,), (1,)), ((), ()))
NN = (((1,), (0,)), ((), ()))
LIMIT = pltpu.CompilerParams(vmem_limit_bytes=16 * 2**20)


def refined(mesh):
    return Mesh(mesh.devices.reshape(2, 6, 2, 4, 2, 4), WAVE + ("lev",))


def dot(a, b, dims):
    return lax.dot_general(a, b, dims, preferred_element_type=jnp.float32)


def damping_table(level_gain, wavenumbers, total_n):
    scaled = (wavenumbers * (wavenumbers + 1)).astype(jnp.float32) / jnp.float32(
        (total_n - 1) * total_n
    )
    return 1.0 / (1.0 + level_gain[:, None] * scaled[None, :] ** 2)


def pack_matrix(m_ref, o_ref):
    m = m_ref[...].astype(jnp.float32)
    o_ref[0:136, :] = m[:, 0:128].astype(jnp.bfloat16)
    tail = m[:, 128:136]
    flipped = jnp.concatenate([tail, jnp.zeros((120, 8), jnp.float32)], axis=0)
    flipped = jnp.concatenate([flipped, jnp.zeros((256, 120), jnp.float32)], axis=1).T
    o_ref[136:152, :] = jnp.concatenate(
        [flipped[0:8, 0:128], flipped[0:8, 128:256]], axis=0
    ).astype(jnp.bfloat16)


def prepare_kernel(x_hbm, m_hbm, o_hbm, p_ref, x_ref, m_ref, o_ref, pairs, sems):
    load_m = pltpu.make_async_copy(m_hbm, m_ref, sems.at[0])
    load_m.start()
    load_x = pltpu.make_async_copy(x_hbm, x_ref, sems.at[1])
    load_x.start()
    load_m.wait()
    pack_matrix(m_ref, p_ref)
    load_x.wait()
    leaving = []
    for h in range(2):
        for c in range(2):
            x = x_ref[:, :, :, h * 384 : h * 384 + 384].astype(jnp.float32)
            rows = jnp.concatenate(
                [x[0, :, c, :], x[1, :, c, :], jnp.zeros((4, 384), jnp.float32)], axis=0
            )
            pairs[h, pl.ds(c, 384, 2), 0:68] = rows.T[:, 0:68]
        both = pairs[h, :, 0:68].astype(jnp.bfloat16).reshape(2, 2, 6, 2, 4, 2, 2, 68)
        for l in range(2):
            for yh in range(2):
                for zh in range(6):
                    for zl in range(2):
                        o_ref[yh, zl, :, 2 * h + l, zh] = both[l, yh, zh, zl]
        part = pl.ds(2 * h, 2)
        leave = pltpu.make_async_copy(
            o_ref.at[:, :, :, part], o_hbm.at[:, :, :, part], sems.at[2 + h]
        )
        leave.start()
        leaving.append(leave)
    for leave in leaving:
        leave.wait()


def solve_kernel(x_ref, m_ref, c_ref, o_hbm, stage, sol, o_ref, pairs, sems):
    nz = m_ref.shape[0]
    for z in range(nz):
        parts = ([], [])
        for l in range(4):
            pairs[z * 4 + l, :, 0:68] = x_ref[:, l, z].reshape(32, 68).astype(jnp.float32)
            for c in range(2):
                parts[c].append(pairs[z * 4 + l, pl.ds(c, 16, 2), :])
        x = jnp.concatenate(
            [
                jnp.concatenate(
                    [parts[c][l][:, r * 34 : r * 34 + 34] for l in range(4)], axis=1
                )
                for c in range(2)
                for r in range(2)
            ],
            axis=0,
        ).astype(jnp.bfloat16)
        tail = m_ref[z, 136:152, :]
        x_tail = x[:, 128:136]
        low = dot(x[:, 0:128], m_ref[z, 0:136, :], NT)
        high = jnp.concatenate(
            [dot(x_tail, tail[0:8, :], NN), dot(x_tail, tail[8:16, 0:8], NN)], axis=1
        )
        sol[z * 64 : z * 64 + 64, :] = (low + high).astype(jnp.bfloat16)
    coupled = dot(sol[...], c_ref[...], NT).astype(jnp.bfloat16)
    for z in range(nz):
        both = [
            values[z * 64 : z * 64 + 64, :].astype(jnp.float32) for values in (sol, coupled)
        ]
        for c in range(2):
            for l in range(4):
                stage[l, c, :, z * 136 : z * 136 + 136] = jnp.concatenate(
                    [
                        values[(c * 2 + r) * 16 : (c * 2 + r) * 16 + 16, l * 34 : l * 34 + 34]
                        for values in both
                        for r in range(2)
                    ],
                    axis=1,
                )
    leaving = []
    for l in range(4):
        for t in range(13):
            for c in range(2):
                tile = stage[l, c, :, t * 128 : t * 128 + 128]
                if t == 12:
                    tile = jnp.concatenate(
                        [tile[:, 0:96], jnp.zeros((16, 32), jnp.float32)], axis=1
                    )
                pairs[l * 13 + t, pl.ds(c, 16, 2), :] = tile
            o_ref[:, l, :, t * 128 : t * 128 + 128] = (
                pairs[l * 13 + t].astype(jnp.bfloat16).reshape(16, 2, 128)
            )
        leave = pltpu.make_async_copy(o_ref.at[:, l], o_hbm.at[:, l], sems.at[l])
        leave.start()
        leaving.append(leave)
    for leave in leaving:
        leave.wait()


def place_kernel(q_ref):
    for g in range(3):
        row = lax.broadcasted_iota(jnp.int32, (256, 768), 0)
        col = lax.broadcasted_iota(jnp.int32, (256, 768), 1)
        q, s, l = 4 * g + (row >> 6), (row >> 2) & 15, row & 3
        yh, zl, x = s >> 3, (s >> 2) & 1, s & 3
        place = l * 192 + yh * 96 + (q >> 1) * 16 + zl * 8 + x * 2 + (q & 1)
        q_ref[g * 256 : g * 256 + 256, :] = jnp.where(col == place, 1.0, 0.0).astype(
            jnp.bfloat16
        )


def finish_kernel(
    m_ref, b_ref, heat_ref, q_ref, div_hbm, temp_hbm, stage, div_ref, temp_ref, sems
):
    full = b_ref[...].astype(jnp.float32)
    spans = []
    for c in range(2):
        flipped = full[:, c, :].T
        spans.append([flipped[q * 136 : (q + 1) * 136, :] for q in range(12)])
    total = None
    for g in range(3):
        sides = [jnp.concatenate(spans[c][4 * g : 4 * g + 4], axis=1) for c in range(2)]
        left = jnp.concatenate(sides, axis=0).astype(jnp.bfloat16)
        part = dot(left, q_ref[g * 256 : g * 256 + 256, :], NN)
        total = part if total is None else total + part
    for c in range(2):
        for t in range(6):
            stage[t, pl.ds(c, 136, 2), :] = total[
                c * 136 : (c + 1) * 136, t * 128 : (t + 1) * 128
            ]
    lane = lax.broadcasted_iota(jnp.int32, (2, 768), 1)
    leaving = []
    for r in range(2):
        inside = lane >= m_ref[r]
        for k in range(34):
            at = 2 * (r * 34 + k)
            solved, coupled = (
                jnp.concatenate([stage[t, i : i + 2, :] for t in range(6)], axis=1)
                for i in (at, 136 + at)
            )
            heat = heat_ref[r, k].astype(jnp.float32)
            div_ref[r, k] = jnp.where(inside, solved, 0.0).astype(jnp.bfloat16)
            temp_ref[r, k] = jnp.where(inside, heat - coupled, 0.0).astype(jnp.bfloat16)
        for f, (ready, out) in enumerate(((div_ref, div_hbm), (temp_ref, temp_hbm))):
            leave = pltpu.make_async_copy(ready.at[r], out.at[r], sems.at[2 * r + f])
            leave.start()
            leaving.append(leave)
    for leave in leaving:
        leave.wait()


VMEM = pl.BlockSpec(memory_space=pltpu.VMEM)
SMEM = pl.BlockSpec(memory_space=pltpu.SMEM)
HBM = pl.BlockSpec(memory_space=pltpu.HBM)


def copies(n):
    return pltpu.SemaphoreType.DMA((n,))


def on_device(
    spin_tendency,
    spreading_source,
    heat_source,
    helmholtz_inverses,
    heat_spreading_coupler,
    smoothing_strengths,
    azimuthal_order_list,
):
    rows, parts, lev_local, total_n = spreading_source.shape
    nyh, nzh, nzl, nx, nc = (lax.axis_size(a) for a in WAVE)
    nlev = lax.axis_size("lev")
    peers = nyh * nzl * nx
    shared = nzh * nc
    layers = lev_local * nlev
    zero = jnp.zeros((), jnp.bfloat16)

    def bf16(*shape):
        return jax.ShapeDtypeStruct(shape, jnp.bfloat16)

    def room(*shape, dtype=jnp.bfloat16):
        return pltpu.VMEM(shape, dtype)

    outgoing = (nyh, nzl, nx, nlev, nzh, nc, parts, rows * lev_local)
    sent, packed = pl.pallas_call(
        prepare_kernel,
        out_shape=(bf16(*outgoing), bf16(layers + 16, 128)),
        in_specs=[HBM, HBM],
        out_specs=(HBM, VMEM),
        scratch_shapes=[
            room(rows, lev_local, parts, total_n),
            room(layers, layers),
            room(*outgoing),
            room(2, parts * total_n // 2, 128, dtype=jnp.float32),
            copies(4),
        ],
        compiler_params=LIMIT,
    )(
        pltpu.with_memory_space_constraint(spreading_source.transpose(0, 2, 1, 3), pltpu.HBM),
        pltpu.with_memory_space_constraint(helmholtz_inverses[0, 0], pltpu.HBM),
    )
    sent = sent.reshape(peers * nlev, shared, parts, rows * lev_local)
    got = lax.all_to_all(sent, PEERS, split_axis=0, concat_axis=0, tiled=True)
    matrices = lax.all_gather(packed, SHARERS, axis=0, tiled=False)

    width = 13 * 128
    both = pl.pallas_call(
        solve_kernel,
        out_shape=bf16(peers, nlev, parts, width),
        in_specs=[VMEM] * 3,
        out_specs=HBM,
        scratch_shapes=[
            room(nlev, parts, peers, width, dtype=jnp.float32),
            room(shared * parts * rows * peers, layers),
            room(peers, nlev, parts, width),
            room(nlev * 13, parts * peers, 128, dtype=jnp.float32),
            copies(4),
        ],
        compiler_params=LIMIT,
    )(
        got.reshape(peers, nlev, shared, parts, rows * lev_local),
        matrices,
        heat_spreading_coupler,
    )
    both = both.reshape(peers * nlev, parts, width)
    back = lax.all_to_all(both, PEERS, split_axis=0, concat_axis=0, tiled=True)

    places = pl.pallas_call(
        place_kernel, out_shape=bf16(total_n, total_n), out_specs=VMEM, compiler_params=LIMIT
    )()
    spectrum = (rows, lev_local, parts, total_n)
    divergence, temperature = pl.pallas_call(
        finish_kernel,
        out_shape=(bf16(*spectrum), bf16(*spectrum)),
        in_specs=[SMEM] + [VMEM] * 3,
        out_specs=(HBM, HBM),
        scratch_shapes=[
            room(total_n // 128, 4 * rows * lev_local, 128, dtype=jnp.float32),
            room(*spectrum),
            room(*spectrum),
            copies(4),
        ],
        compiler_params=LIMIT,
    )(azimuthal_order_list, back, heat_source.transpose(0, 2, 1, 3), places)

    level_gain = lax.dynamic_slice_in_dim(
        smoothing_strengths, lax.axis_index("lev") * lev_local, lev_local
    )
    damping = damping_table(level_gain, jnp.arange(total_n, dtype=jnp.int32), total_n)
    spin_updated = (spin_tendency.astype(jnp.float32) * damping[None, None]).astype(jnp.bfloat16)
    interior = (
        jnp.arange(total_n, dtype=jnp.int32)[None, :] >= azimuthal_order_list[:, None]
    )[:, None, None, :]
    return (
        jnp.where(interior, spin_updated, zero),
        divergence.transpose(0, 2, 1, 3),
        temperature.transpose(0, 2, 1, 3),
    )


def solution(mesh):
    spectrum = P(WAVE, None, "lev", None)
    return jax.shard_map(
        on_device,
        mesh=refined(mesh),
        in_specs=(spectrum, spectrum, spectrum, P("lev", WAVE, None, None), P(), P(), P(WAVE)),
        out_specs=(spectrum,) * 3,
        check_vma=False,
    )
```
